32 devices in a mesh: dp: 1 (over z), pp: 4 (over y), ep: 8 (over x, core).
Axes of the slice: x: 4, y: 4, z: 1, core: 2. Of those that a mesh axis runs over, the one named last changes fastest.
The devices are a block of a 4x4x8 slice.
Arguments:
- hidden_in: bfloat16 [24, 128, 1536], P(None, ('dp', 'ep'))
- seq_pos: int32 [24, 128], P(None, ('dp', 'ep'))
- k_cache: bfloat16 [4, 24, 128, 16, 8, 64], P('pp', None, ('dp', 'ep'))
- v_cache: bfloat16 [4, 24, 128, 16, 8, 64], P('pp', None, ('dp', 'ep'))
- expert_ids: int32 [4, 24, 128, 8], P('pp', None, ('dp', 'ep'))
- w_query: bfloat16 [4, 1536, 1536], P('pp')
- w_key: bfloat16 [4, 1536, 512], P('pp')
- w_value: bfloat16 [4, 1536, 512], P('pp')
- w_out: bfloat16 [4, 1536, 1536], P('pp')
- attn_gain: bfloat16 [4, 1536], P('pp')
- mlp_gain: bfloat16 [4, 1536], P('pp')
- w_router: bfloat16 [4, 1536, 40], P('pp')
- w_gate: bfloat16 [4, 40, 1536, 512], P('pp', 'ep')
- w_up: bfloat16 [4, 40, 1536, 512], P('pp', 'ep')
- w_down: bfloat16 [4, 40, 512, 1536], P('pp', 'ep')
- final_gain: bfloat16 [1536], replicated
Outputs:
- output 1: bfloat16 [24, 128, 1536], P(None, ('dp', 'ep'))
- output 2: bfloat16 [4, 24, 128, 8, 64], P('pp', None, ('dp', 'ep'))
- output 3: bfloat16 [4, 24, 128, 8, 64], P('pp', None, ('dp', 'ep'))
All inputs are finite; a program needn't handle non-finite values.
Results may differ from the reference program's by a relative error of at most 0.02.
Values are sent between devices in bfloat16 or wider.
A program may use at most 768 MiB of HBM per device.

```python
import jax
import jax.numpy as jnp
from jax import lax

D = 1536
HEADS = 24
KV_HEADS = 8
HEAD = 64
EXPERTS = 40
FF = 512
TOP = 8
LAYERS = 4
EP_SIZE = 8
MICRO_COUNT = 24
TOK_DEV = 16
CONTEXT = 16
MICRO_ROWS = EP_SIZE * TOK_DEV
LOCAL_EXPERTS = EXPERTS // EP_SIZE
THETA = 1000000.0
EPS = 1e-05


def draw_routes(route_key):
    hot_key, perm_key, local_key = jax.random.split(route_key, 3)
    hot_dev = jax.random.randint(hot_key, (LAYERS, MICRO_COUNT, 1, 1), 0, EP_SIZE)
    perm_keys = jax.random.split(perm_key, LAYERS * MICRO_COUNT * EP_SIZE)
    slot_pos = jax.vmap(lambda one_key: jax.random.permutation(one_key, TOK_DEV))(perm_keys)
    slot_pos = slot_pos.reshape(LAYERS, MICRO_COUNT, EP_SIZE, TOK_DEV)
    first_dev = jnp.where(slot_pos < TOK_DEV // 2, hot_dev, (hot_dev + slot_pos) % EP_SIZE)
    local_base = jax.random.randint(local_key, (LAYERS, MICRO_COUNT, EP_SIZE, TOK_DEV, 1), 0, LOCAL_EXPERTS)
    choice = jnp.arange(TOP)
    dest_dev = (first_dev[..., None] + choice) % EP_SIZE
    local_idx = (local_base + choice // EP_SIZE) % LOCAL_EXPERTS
    route_ids = dest_dev * LOCAL_EXPERTS + local_idx
    return route_ids.reshape(LAYERS, MICRO_COUNT, MICRO_ROWS, TOP).astype(jnp.int32)


def draw_normal(one_key, arr_shape, std_scale):
    return (jax.random.normal(one_key, arr_shape, jnp.float32) * std_scale).astype(jnp.bfloat16)


def draw_gain(one_key, arr_shape):
    return (1.0 + 0.3 * jax.random.normal(one_key, arr_shape, jnp.float32)).astype(jnp.bfloat16)


def setup_inputs(seed: int = 0, part: int = 0) -> dict:
    shared_keys = jax.random.split(jax.random.key(seed), 11)
    part_keys = jax.random.split(jax.random.fold_in(jax.random.key(seed + 1), part), 5)
    pos_draw = jax.random.randint(part_keys[1], (MICRO_COUNT, MICRO_ROWS), 1, CONTEXT + 1)
    first_row = jnp.arange(MICRO_COUNT * MICRO_ROWS).reshape(MICRO_COUNT, MICRO_ROWS) == 0
    seq_pos = jnp.where(first_row, CONTEXT, pos_draw).astype(jnp.int32)
    cache_shape = (LAYERS, MICRO_COUNT, MICRO_ROWS, CONTEXT, KV_HEADS, HEAD)
    out_scale = 0.5 * (CONTEXT ** 0.5) * (HEADS * HEAD) ** -0.5
    return {
        "hidden_in": draw_normal(part_keys[0], (MICRO_COUNT, MICRO_ROWS, D), 1.0),
        "seq_pos": seq_pos,
        "k_cache": draw_normal(part_keys[2], cache_shape, 1.0),
        "v_cache": draw_normal(part_keys[3], cache_shape, 1.0),
        "expert_ids": draw_routes(part_keys[4]),
        "w_query": draw_normal(shared_keys[0], (LAYERS, D, HEADS * HEAD), D ** -0.5),
        "w_key": draw_normal(shared_keys[1], (LAYERS, D, KV_HEADS * HEAD), D ** -0.5),
        "w_value": draw_normal(shared_keys[2], (LAYERS, D, KV_HEADS * HEAD), D ** -0.5),
        "w_out": draw_normal(shared_keys[3], (LAYERS, HEADS * HEAD, D), out_scale),
        "attn_gain": draw_gain(shared_keys[4], (LAYERS, D)),
        "mlp_gain": draw_gain(shared_keys[5], (LAYERS, D)),
        "w_router": draw_normal(shared_keys[6], (LAYERS, D, EXPERTS), 2.0 * D ** -0.5),
        "w_gate": draw_normal(shared_keys[7], (LAYERS, EXPERTS, D, FF), D ** -0.5),
        "w_up": draw_normal(shared_keys[8], (LAYERS, EXPERTS, D, FF), D ** -0.5),
        "w_down": draw_normal(shared_keys[9], (LAYERS, EXPERTS, FF, D), FF ** -0.5),
        "final_gain": draw_gain(shared_keys[10], (D,)),
    }


def rms_norm(in_vals, gain_vec):
    vals_f32 = in_vals.astype(jnp.float32)
    inv_rms = lax.rsqrt(jnp.mean(vals_f32 * vals_f32, axis=-1, keepdims=True) + EPS)
    return (vals_f32 * inv_rms * gain_vec.astype(jnp.float32)).astype(jnp.bfloat16)


def rotate(head_vecs, positions):
    half_dim = head_vecs.shape[-1] // 2
    inv_freq = THETA ** (-jnp.arange(half_dim, dtype=jnp.float32) / half_dim)
    angles = positions.astype(jnp.float32)[:, None, None] * inv_freq
    cos_ang = jnp.cos(angles)
    sin_ang = jnp.sin(angles)
    first_half = head_vecs[..., :half_dim].astype(jnp.float32)
    second_half = head_vecs[..., half_dim:].astype(jnp.float32)
    return jnp.concatenate([first_half * cos_ang - second_half * sin_ang, second_half * cos_ang + first_half * sin_ang], axis=-1).astype(jnp.bfloat16)


def attend(q_heads, key_new, val_new, k_rows, v_rows, positions):
    tokens = key_new.shape[0]
    q_groups = q_heads.reshape(tokens, KV_HEADS, HEADS // KV_HEADS, HEAD).astype(jnp.float32)
    score_scale = HEAD ** -0.5
    cache_scores = jnp.einsum("bkgh,btkh->bkgt", q_groups, k_rows.astype(jnp.float32)) * score_scale
    is_valid = jnp.arange(CONTEXT)[None, None, None, :] < positions[:, None, None, None]
    cache_scores = jnp.where(is_valid, cache_scores, -jnp.inf)
    self_score = jnp.einsum("bkgh,bkh->bkg", q_groups, key_new.astype(jnp.float32))[..., None] * score_scale
    top_score = jnp.maximum(jnp.max(cache_scores, axis=-1, keepdims=True), self_score)
    cache_w = jnp.exp(cache_scores - top_score)
    self_w = jnp.exp(self_score - top_score)
    weight_sum = jnp.sum(cache_w, axis=-1, keepdims=True) + self_w
    cache_w = (cache_w / weight_sum).astype(jnp.bfloat16).astype(jnp.float32)
    self_w = (self_w / weight_sum).astype(jnp.bfloat16).astype(jnp.float32)
    attn_out = jnp.einsum("bkgt,btkh->bkgh", cache_w, v_rows.astype(jnp.float32)) + self_w * val_new.astype(jnp.float32)[:, :, None, :]
    return attn_out.astype(jnp.bfloat16).reshape(tokens, HEADS * HEAD)


def one_micro(hidden, positions, k_rows, v_rows, choice_ids, layer_w):
    w_q, w_k, w_v, w_o, a_gain, m_gain, w_r, w_g, w_u, w_d = layer_w
    tokens = hidden.shape[0]
    normed = rms_norm(hidden, a_gain)
    q_heads = jnp.dot(normed, w_q, preferred_element_type=jnp.float32).astype(jnp.bfloat16).reshape(tokens, HEADS, HEAD)
    key_new = jnp.dot(normed, w_k, preferred_element_type=jnp.float32).astype(jnp.bfloat16).reshape(tokens, KV_HEADS, HEAD)
    val_new = jnp.dot(normed, w_v, preferred_element_type=jnp.float32).astype(jnp.bfloat16).reshape(tokens, KV_HEADS, HEAD)
    q_heads = rotate(q_heads, positions)
    key_new = rotate(key_new, positions)
    attn_out = attend(q_heads, key_new, val_new, k_rows, v_rows, positions)
    hidden = (hidden.astype(jnp.float32) + jnp.dot(attn_out, w_o, preferred_element_type=jnp.float32)).astype(jnp.bfloat16)
    normed = rms_norm(hidden, m_gain)
    logits = jnp.dot(normed, w_r, preferred_element_type=jnp.float32)
    gate_vals = jax.nn.softmax(jnp.take_along_axis(logits, choice_ids, axis=1), axis=-1)
    coef_mat = jnp.sum(gate_vals[:, :, None] * (choice_ids[:, :, None] == jnp.arange(EXPERTS)[None, None, :]), axis=1)

    def expert_body(acc_sum, expert_args):
        gate_w, up_w, down_w, coef_col = expert_args
        act_rows = (jax.nn.silu(jnp.dot(normed, gate_w, preferred_element_type=jnp.float32)) * jnp.dot(normed, up_w, preferred_element_type=jnp.float32)).astype(jnp.bfloat16)
        down_h = jnp.dot(act_rows, down_w, preferred_element_type=jnp.float32)
        return acc_sum + (coef_col[:, None] * down_h).astype(jnp.bfloat16).astype(jnp.float32), None

    moe_sum, _ = lax.scan(expert_body, jnp.zeros(hidden.shape, jnp.float32), (w_g, w_u, w_d, coef_mat.T))
    hidden = (hidden.astype(jnp.float32) + moe_sum.astype(jnp.bfloat16).astype(jnp.float32)).astype(jnp.bfloat16)
    return hidden, key_new, val_new


def reference(hidden_in, seq_pos, k_cache, v_cache, expert_ids, w_query, w_key, w_value, w_out, attn_gain, mlp_gain, w_router, w_gate, w_up, w_down, final_gain):
    def layer_body(hidden, layer_args):
        layer_w = layer_args[3:]

        def micro_body(micro_args):
            return one_micro(micro_args[0], micro_args[1], micro_args[2], micro_args[3], micro_args[4], layer_w)

        hidden, k_rows, v_rows = lax.map(micro_body, (hidden, seq_pos, layer_args[0], layer_args[1], layer_args[2]))
        return hidden, (k_rows, v_rows)

    hidden, new_rows = lax.scan(layer_body, hidden_in, (k_cache, v_cache, expert_ids, w_query, w_key, w_value, w_out, attn_gain, mlp_gain, w_router, w_gate, w_up, w_down))
    return rms_norm(hidden, final_gain), new_rows[0], new_rows[1]
```

```python
import functools

import jax
import jax.numpy as jnp
from jax import lax
from jax.experimental import pallas as pl
from jax.experimental.pallas import tpu as pltpu
from jax.sharding import PartitionSpec as P

THETA = 1000000.0
EPS = 1e-05
GROUP = 2
SLOTS = 3
MESH = pl.DeviceIdType.MESH
BF16 = jnp.bfloat16
F32 = jnp.float32


def rms(vals_f32, gain_f32):
    inv_rms = lax.rsqrt(jnp.mean(vals_f32 * vals_f32, axis=-1, keepdims=True) + EPS)
    return (vals_f32 * inv_rms * gain_f32).astype(BF16)


def mm(a, b):
    return jnp.dot(a, b, preferred_element_type=F32)


def kernel(cfg, pos_ref, hid_hbm, cos_ref, sin_ref, msk_hbm, kc_hbm, vc_hbm,
           wq_hbm, wk_hbm, wv_hbm, wo_hbm, wg_hbm, wu_hbm, wd_hbm, wr_ref, ag_ref, mg_ref, fg_ref,
           out_hbm, kn_ref, vn_ref,
           wqkv, wo, wg, wu, wd, h_buf, h_out, h_mid, rows_buf, msk_all,
           acc, pair_buf, c_send, c_own, c_recv, kbuf, vbuf, qkv_s, q_ht, o_s, act_s, perm, rep,
           w_sem, we_sem, hin_sem, kv_sem, own_sem, msk_send, msk_recv,
           ag_send, ag_recv, fw_send, pr_send, pr_recv, cs_send, cs_recv,
           h_send, h_recv, f_send, f_recv, f_loc):
    steps, rows, width, ep_size, pp_size, heads, kv_heads, head, ctx, toks, local_e = cfg
    chips = ep_size // 2
    dp_i, stage, me = lax.axis_index("dp"), lax.axis_index("pp"), lax.axis_index("ep")
    core = lax.rem(me, 2)
    chip = me // 2
    partner = me + 1 - 2 * core
    last = pp_size - 1
    micros = rows // toks
    kvw = kv_heads * head
    qw = heads * head
    rep_n = heads // kv_heads
    hrows = toks * heads
    tpc = 256 // (ctx * kv_heads)
    cols = tpc * ctx * kv_heads
    crows = tpc * heads

    def ep_id(idx):
        return (dp_i, stage, idx)

    def same_core(dx):
        return 2 * lax.rem(chip + dx, chips) + core

    barrier = pltpu.get_barrier_semaphore()
    for d in range(1, ep_size):
        pl.semaphore_signal(barrier, inc=1, device_id=ep_id(lax.rem(me + d, ep_size)), device_id_type=MESH)
    for d in range(1, pp_size):
        pl.semaphore_signal(barrier, inc=1, device_id=(dp_i, lax.rem(stage + d, pp_size), me), device_id_type=MESH)

    def wcopies():
        return [pltpu.make_async_copy(wq_hbm, wqkv.at[:, pl.ds(0, qw)], w_sem.at[0]),
                pltpu.make_async_copy(wk_hbm, wqkv.at[:, pl.ds(qw, kvw)], w_sem.at[1]),
                pltpu.make_async_copy(wv_hbm, wqkv.at[:, pl.ds(qw + kvw, kvw)], w_sem.at[2]),
                pltpu.make_async_copy(wo_hbm, wo, w_sem.at[3])]

    def ecopies(e):
        return [pltpu.make_async_copy(wg_hbm.at[e], wg.at[e], we_sem.at[0, e]),
                pltpu.make_async_copy(wu_hbm.at[e], wu.at[e], we_sem.at[1, e]),
                pltpu.make_async_copy(wd_hbm.at[e], wd.at[e], we_sem.at[2, e])]

    def kv_copies(i, slot):
        return [pltpu.make_async_copy(kc_hbm.at[i], kbuf.at[slot], kv_sem.at[0, slot]),
                pltpu.make_async_copy(vc_hbm.at[i], vbuf.at[slot], kv_sem.at[1, slot])]

    hin = pltpu.make_async_copy(hid_hbm, h_buf, hin_sem)
    own_msk = pltpu.make_async_copy(msk_hbm, msk_all.at[me], own_sem)

    @pl.when(stage == 0)
    def _():
        hin.start()

    wc = wcopies()
    wc[0].start()
    wc[1].start()
    wc[2].start()
    for cp in kv_copies(0, 0):
        cp.start()
    wc[3].start()
    own_msk.start()
    for e in range(local_e):
        for cp in ecopies(e):
            cp.start()

    r0 = lax.broadcasted_iota(jnp.int32, (hrows, hrows), 0)
    r1 = lax.broadcasted_iota(jnp.int32, (hrows, hrows), 1)
    perm[...] = jnp.where((r0 // heads == r1 % toks) & (r0 % heads == r1 // toks), 1.0, 0.0).astype(BF16)
    s0 = lax.broadcasted_iota(jnp.int32, (hrows, kv_heads * toks), 0)
    s1 = lax.broadcasted_iota(jnp.int32, (hrows, kv_heads * toks), 1)
    rep[...] = jnp.where((s0 // heads == s1 % toks) & ((s0 % heads) // rep_n == s1 // toks), 1.0, 0.0).astype(BF16)

    pl.semaphore_wait(barrier, ep_size - 1 + pp_size - 1)

    def msk_copy(d):
        return pltpu.make_async_remote_copy(
            src_ref=msk_hbm, dst_ref=msk_all.at[me], send_sem=msk_send.at[d], recv_sem=msk_recv.at[d],
            device_id=ep_id(lax.rem(me + d, ep_size)), device_id_type=MESH)

    for d in range(1, ep_size):
        msk_copy(d).start()

    def ag_copy(j, dx):
        slot = lax.rem(j, SLOTS)
        return pltpu.make_async_remote_copy(
            src_ref=rows_buf.at[slot, me], dst_ref=rows_buf.at[slot, me],
            send_sem=ag_send.at[slot, dx], recv_sem=ag_recv.at[slot, dx],
            device_id=ep_id(partner if dx == 0 else same_core(dx)), device_id_type=MESH)

    def fw_copy(j, dx):
        slot = lax.rem(j, SLOTS)
        src = same_core(chips - dx)
        return pltpu.make_async_remote_copy(
            src_ref=rows_buf.at[slot, src], dst_ref=rows_buf.at[slot, src],
            send_sem=fw_send.at[slot, dx], recv_sem=ag_recv.at[slot, chips + dx],
            device_id=ep_id(partner), device_id_type=MESH)

    def pair_copy(j, x):
        slot = lax.rem(j, 2)
        return pltpu.make_async_remote_copy(
            src_ref=acc.at[2 * x + 1 - core], dst_ref=pair_buf.at[slot, x],
            send_sem=pr_send.at[x], recv_sem=pr_recv.at[slot, x],
            device_id=ep_id(partner), device_id_type=MESH)

    def c_copy(j, dx):
        slot = lax.rem(j, SLOTS)
        return pltpu.make_async_remote_copy(
            src_ref=c_send.at[dx - 1], dst_ref=c_recv.at[slot, dx - 1],
            send_sem=cs_send.at[dx - 1], recv_sem=cs_recv.at[slot, dx - 1],
            device_id=ep_id(same_core(dx)), device_id_type=MESH)

    def h_copy(j):
        return pltpu.make_async_remote_copy(
            src_ref=h_out.at[j], dst_ref=h_buf.at[j], send_sem=h_send.at[j], recv_sem=h_recv.at[j],
            device_id=(dp_i, lax.rem(stage + 1, pp_size), me), device_id_type=MESH)

    def f_copy(j, d):
        return pltpu.make_async_remote_copy(
            src_ref=h_out.at[j], dst_ref=out_hbm.at[j], send_sem=f_send.at[j, d - 1], recv_sem=f_recv.at[j],
            device_id=(dp_i, lax.rem(stage + d, pp_size), me), device_id_type=MESH)

    def f_local(j):
        return pltpu.make_async_copy(h_out.at[j], out_hbm.at[j], f_loc.at[j])

    lane128 = lax.broadcasted_iota(jnp.int32, (rows, 128), 1)
    low_half = lane128 % head < head // 2
    sc_row = lax.broadcasted_iota(jnp.int32, (crows, cols), 0)
    sc_col = lax.broadcasted_iota(jnp.int32, (crows, cols), 1)
    sc_tok = sc_row // heads
    sc_same = (sc_tok == sc_col // (ctx * kv_heads)) & ((sc_row % heads) // rep_n == sc_col % kv_heads)
    sc_ctx = (sc_col // kv_heads) % ctx
    scale = head ** -0.5

    def attention(i):
        kslot = lax.rem(i, 2)

        @pl.when(i + 1 < steps)
        def _():
            for cp in kv_copies(i + 1, 1 - kslot):
                cp.start()

        @pl.when((i == 0) & (stage == 0))
        def _():
            hin.wait()

        @pl.when(stage > 0)
        def _():
            h_copy(i).wait_recv()

        @pl.when(i == 0)
        def _():
            wc[0].wait()
            wc[1].wait()
            wc[2].wait()

        hid = h_buf[i].astype(F32)
        normed = rms(hid, ag_ref[...].astype(F32))
        cos = cos_ref[i]
        sin = sin_ref[i]
        span = 512
        for n in range((qw + 2 * kvw) // span):
            blk = mm(normed, wqkv[:, n * span:(n + 1) * span]).astype(BF16).astype(F32)
            for b in range(span // 128):
                at = n * span + b * 128
                piece = blk[:, b * 128:(b + 1) * 128]
                if at < qw + kvw:
                    swap = jnp.where(low_half, pltpu.roll(piece, 128 - head // 2, 1), pltpu.roll(piece, head // 2, 1))
                    piece = piece * cos + swap * sin
                piece16 = piece.astype(BF16)
                if at < qw:
                    base = at // head * toks
                    for m in range(micros):
                        for p in range(128 // head):
                            q_ht[m, base + p * toks:base + (p + 1) * toks, :] = piece16[m * toks:(m + 1) * toks, p * head:(p + 1) * head]
                else:
                    if at < qw + kvw:
                        kn_ref[i, :, at - qw:at - qw + 128] = piece16
                    else:
                        vn_ref[i, :, at - qw - kvw:at - qw - kvw + 128] = piece16
                    base = hrows + (at - qw) // head * toks
                    for m in range(micros):
                        for p in range(128 // head):
                            q_ht[m, base + p * toks:base + (p + 1) * toks, :] = piece16[m * toks:(m + 1) * toks, p * head:(p + 1) * head]

        for cp in kv_copies(i, kslot):
            cp.wait()
        krows = kv_heads * toks
        for m in range(micros):
            q_th = mm(perm[...], q_ht[m, 0:hrows, :]).astype(BF16)
            k_rep = mm(rep[...], q_ht[m, hrows:hrows + krows, :])
            v_rep = mm(rep[...], q_ht[m, hrows + krows:hrows + 2 * krows, :])
            own = jnp.sum(q_th.astype(F32) * k_rep, axis=-1, keepdims=True) * scale
            outs = []
            for c in range(toks // tpc):
                kt = kbuf[kslot, m * toks * ctx * kv_heads + c * cols:m * toks * ctx * kv_heads + (c + 1) * cols, :]
                vt = vbuf[kslot, m * toks * ctx * kv_heads + c * cols:m * toks * ctx * kv_heads + (c + 1) * cols, :]
                s = lax.dot_general(q_th[c * crows:(c + 1) * crows], kt, (((1,), (1,)), ((), ())), preferred_element_type=F32) * scale
                posv = pos_ref[i * micros + m, c * tpc]
                for t in range(1, tpc):
                    posv = jnp.where(sc_tok == t, pos_ref[i * micros + m, c * tpc + t], posv)
                s = jnp.where(sc_same & (sc_ctx < posv), s, -jnp.inf)
                own_c = own[c * crows:(c + 1) * crows]
                top = jnp.maximum(jnp.max(s, axis=-1, keepdims=True), own_c)
                w = jnp.exp(s - top)
                own_w = jnp.exp(own_c - top)
                total = jnp.sum(w, axis=-1, keepdims=True) + own_w
                w = (w / total).astype(BF16)
                own_w = (own_w / total).astype(BF16).astype(F32)
                outs.append((mm(w, vt) + own_w * v_rep[c * crows:(c + 1) * crows]).astype(BF16))
            o_th = jnp.concatenate(outs, axis=0)
            o_ht = lax.dot_general(perm[...], o_th, (((0,), (0,)), ((), ())), preferred_element_type=F32)
            for b in range(qw // 128):
                pieces = [o_ht[(b * (128 // head) + p) * toks:(b * (128 // head) + p + 1) * toks, :] for p in range(128 // head)]
                o_s[m * toks:(m + 1) * toks, b * 128:(b + 1) * 128] = jnp.concatenate(pieces, axis=1).astype(BF16)

        @pl.when(i == 0)
        def _():
            wc[3].wait()

        mslot = lax.rem(i, SLOTS)
        attn = o_s[...]
        for n in range(width // span):
            part = mm(attn, wo[:, n * span:(n + 1) * span])
            h_mid[mslot, :, n * span:(n + 1) * span] = (h_buf[i, :, n * span:(n + 1) * span].astype(F32) + part).astype(BF16)
        rows_buf[mslot, me] = rms(h_mid[mslot].astype(F32), mg_ref[...].astype(F32))
        for dx in range(chips):
            ag_copy(i, dx).start()

    def forward(i):
        for dx in range(1, chips):
            ag_copy(i, dx).wait_recv()
            fw_copy(i, dx).start()

    def experts(j):
        slot = lax.rem(j, SLOTS)
        ag_copy(j, 0).wait_recv()
        for dx in range(1, chips):
            fw_copy(j, dx).wait_recv()

        @pl.when(j == 0)
        def _():
            own_msk.wait()
            for d in range(1, ep_size):
                msk_copy(d).wait_recv()

        total = ep_size * rows
        xs = rows_buf[slot].reshape(total, width)
        logits = mm(xs, wr_ref[...])
        chosen = msk_all[:, j].reshape(total, 128).astype(F32) > 0.5
        logits = jnp.where(chosen, logits, -jnp.inf)
        numer = jnp.exp(logits - jnp.max(logits, axis=-1, keepdims=True))
        gates = numer / jnp.sum(numer, axis=-1, keepdims=True)
        lane = lax.broadcasted_iota(jnp.int32, (total, 128), 1)
        ff = wg.shape[2]

        def body(e, carry):
            @pl.when(j == 0)
            def _():
                for cp in ecopies(e):
                    cp.wait()

            col = jnp.sum(jnp.where(lane == me * local_e + e, gates, 0.0), axis=-1, keepdims=True)
            for n in range(ff // 256):
                xv = rows_buf[slot].reshape(total, width)
                gate_h = mm(xv, wg[e, :, n * 256:(n + 1) * 256])
                up_h = mm(xv, wu[e, :, n * 256:(n + 1) * 256])
                act_s[:, n * 256:(n + 1) * 256] = (jax.nn.silu(gate_h) * up_h).astype(BF16)
            for n in range(width // 256):
                part = mm(act_s[...], wd[e, :, n * 256:(n + 1) * 256])
                term = (col * part).astype(BF16).astype(F32).reshape(ep_size, rows, 256)
                old = acc[:, :, n * 256:(n + 1) * 256]
                acc[:, :, n * 256:(n + 1) * 256] = jnp.where(e == 0, term, old + term)
            return carry

        lax.fori_loop(0, local_e, body, 0)
        for x in range(chips):
            pair_copy(j, x).start()

    def pair_sum(j):
        slot = lax.rem(j, 2)
        for dx in range(chips):
            ag_copy(j, dx).wait_send()
            if dx:
                fw_copy(j, dx).wait_send()
        for x in range(chips):
            pair_copy(j, x).wait()
        for dx in range(1, chips):
            x = lax.rem(chip + dx, chips)
            c_send[dx - 1] = acc[2 * x + core] + pair_buf[slot, x]
            c_copy(j, dx).start()
        c_own[...] = acc[me] + pair_buf[slot, chip]

    def finish(j):
        slot = lax.rem(j, SLOTS)
        for dx in range(1, chips):
            c_copy(j, dx).wait()
        total = c_own[...]
        for dx in range(1, chips):
            total = total + c_recv[slot, dx - 1]
        hid = (h_mid[slot].astype(F32) + total.astype(BF16).astype(F32)).astype(BF16)

        @pl.when(stage < last)
        def _():
            h_out[j] = hid
            h_copy(j).start()

        @pl.when(stage == last)
        def _():
            h_out[j] = rms(hid.astype(F32), fg_ref[...].astype(F32))
            for d in range(1, pp_size):
                f_copy(j, d).start()
            f_local(j).start()

    def step(i, carry):
        @pl.when(i < steps)
        def _():
            attention(i)

        @pl.when(i >= 2)
        def _():
            pair_sum(i - 2)

        @pl.when((i >= 1) & (i <= steps))
        def _():
            experts(i - 1)

        @pl.when(i < steps)
        def _():
            forward(i)

        @pl.when(i >= 2)
        def _():
            finish(i - 2)

        return carry

    lax.fori_loop(0, steps + 2, step, 0)

    for d in range(1, ep_size):
        msk_copy(d).wait_send()

    def drain(j, carry):
        @pl.when(stage < last)
        def _():
            h_copy(j).wait_send()
            f_copy(j, 1).wait_recv()

        @pl.when(stage == last)
        def _():
            for d in range(1, pp_size):
                f_copy(j, d).wait_send()
            f_local(j).wait()

        return carry

    lax.fori_loop(0, steps, drain, 0)


def solution(mesh):
    ep_size = mesh.shape["ep"]
    pp_size = mesh.shape["pp"]
    rows_spec = ("dp", "ep")
    three_dim = P("pp", None, None)
    two_dim = P("pp", None)
    expert_spec = P("pp", "ep", None, None)
    cache_spec = P("pp", None, rows_spec, None, None, None)
    new_spec = P("pp", None, rows_spec, None, None)
    in_specs = (P(None, rows_spec, None), P(None, rows_spec), cache_spec, cache_spec, P("pp", None, rows_spec, None), three_dim, three_dim, three_dim, three_dim, two_dim, two_dim, three_dim, expert_spec, expert_spec, expert_spec, P(None))
    out_specs = (P(None, rows_spec, None), new_spec, new_spec)

    def device_fn(hidden_in, seq_pos, k_cache, v_cache, expert_ids, w_query, w_key, w_value, w_out, attn_gain, mlp_gain, w_router, w_gate, w_up, w_down, final_gain):
        assert w_query.shape[0] == 1
        micro_count, toks, width = hidden_in.shape
        ctx, kv_heads, head = k_cache.shape[3:]
        heads = w_query.shape[2] // head
        local_e, ff = w_gate.shape[1], w_gate.shape[3]
        experts = w_router.shape[2]
        kvw, qw = kv_heads * head, heads * head
        steps = micro_count // GROUP
        rows = GROUP * toks
        chips = ep_size // 2
        half = head // 2
        inv_freq = THETA ** (-jnp.arange(half, dtype=F32) / half)
        ang = seq_pos.reshape(steps, rows).astype(F32)[:, :, None] * inv_freq
        cos, sin = jnp.cos(ang), jnp.sin(ang)
        reps = 128 // head
        cos_t = jnp.concatenate([cos, cos] * reps, axis=-1)
        sin_t = jnp.concatenate([-sin, sin] * reps, axis=-1)
        ids = expert_ids[0].reshape(steps, rows, -1)
        chosen = jnp.any(ids[..., :, None] == jnp.arange(128, dtype=jnp.int32), axis=-2).astype(BF16)
        wr = jnp.pad(w_router[0], ((0, 0), (0, 128 - experts)))
        cache_rows = GROUP * toks * ctx * kv_heads
        hrows = toks * heads
        cfg = (steps, rows, width, ep_size, pp_size, heads, kv_heads, head, ctx, toks, local_e)
        vm = pl.BlockSpec(memory_space=pltpu.VMEM)
        hb = pl.BlockSpec(memory_space=pl.ANY)
        dma = pltpu.SemaphoreType.DMA
        call = pl.pallas_call(
            functools.partial(kernel, cfg),
            out_shape=(jax.ShapeDtypeStruct((steps, rows, width), BF16),
                       jax.ShapeDtypeStruct((steps, rows, kvw), BF16),
                       jax.ShapeDtypeStruct((steps, rows, kvw), BF16)),
            in_specs=[pl.BlockSpec(memory_space=pltpu.SMEM), hb, vm, vm, hb, hb, hb] + [hb] * 7 + [vm] * 4,
            out_specs=(hb, vm, vm),
            scratch_shapes=[
                pltpu.VMEM((width, qw + 2 * kvw), BF16), pltpu.VMEM((qw, width), BF16),
                pltpu.VMEM((local_e, width, ff), BF16), pltpu.VMEM((local_e, width, ff), BF16), pltpu.VMEM((local_e, ff, width), BF16),
                pltpu.VMEM((steps, rows, width), BF16), pltpu.VMEM((steps, rows, width), BF16), pltpu.VMEM((SLOTS, rows, width), BF16),
                pltpu.VMEM((SLOTS, ep_size, rows, width), BF16), pltpu.VMEM((ep_size, steps, rows, 128), BF16),
                pltpu.VMEM((ep_size, rows, width), F32), pltpu.VMEM((2, chips, rows, width), F32),
                pltpu.VMEM((chips - 1, rows, width), F32), pltpu.VMEM((rows, width), F32), pltpu.VMEM((SLOTS, chips - 1, rows, width), F32),
                pltpu.VMEM((2, cache_rows, head), BF16), pltpu.VMEM((2, cache_rows, head), BF16),
                pltpu.VMEM((8, 128), F32), pltpu.VMEM((GROUP, hrows + 2 * kv_heads * toks, head), BF16), pltpu.VMEM((rows, qw), BF16),
                pltpu.VMEM((ep_size * rows, ff), BF16), pltpu.VMEM((hrows, hrows), BF16), pltpu.VMEM((hrows, kv_heads * toks), BF16),
                dma((4,)), dma((3, local_e)), dma(()), dma((2, 2)), dma(()), dma((ep_size,)), dma((ep_size,)),
                dma((SLOTS, chips)), dma((SLOTS, 2 * chips)), dma((SLOTS, chips)), dma((chips,)), dma((2, chips)), dma((chips - 1,)), dma((SLOTS, chips - 1)),
                dma((steps,)), dma((steps,)), dma((steps, pp_size - 1)), dma((steps,)), dma((steps,)),
            ],
            compiler_params=pltpu.CompilerParams(collective_id=0, has_side_effects=True, vmem_limit_bytes=66 * 1000 * 1000),
        )
        out, k_new, v_new = call(
            seq_pos, hidden_in.reshape(steps, rows, width), cos_t, sin_t, chosen,
            k_cache.reshape(steps, cache_rows, head), v_cache.reshape(steps, cache_rows, head),
            w_query[0], w_key[0], w_value[0], w_out[0], w_gate[0], w_up[0], w_down[0], wr,
            attn_gain, mlp_gain, final_gain.reshape(1, width))
        new_shape = (1, micro_count, toks, kv_heads, head)
        return out.reshape(micro_count, toks, width), k_new.reshape(new_shape), v_new.reshape(new_shape)

    return jax.shard_map(device_fn, mesh=mesh, in_specs=in_specs, out_specs=out_specs, check_vma=False)
```

```python
import functools

import jax
import numpy as np
import jax.numpy as jnp
from jax import lax
from jax.experimental import pallas as pl
from jax.experimental.pallas import tpu as pltpu
from jax.sharding import PartitionSpec as P

THETA = 1000000.0
EPS = 1e-05
GROUP = 2
SLOTS = 3
PART = 3
CHUNK = 256
MESH = pl.DeviceIdType.MESH
BF16 = jnp.bfloat16
F32 = jnp.float32


def rms(vals_f32, gain_f32):
    inv_rms = lax.rsqrt(jnp.mean(vals_f32 * vals_f32, axis=-1, keepdims=True) + EPS)
    return (vals_f32 * inv_rms * gain_f32).astype(BF16)


def mm(a, b):
    return jnp.dot(a, b, preferred_element_type=F32)


def kernel(cfg, pos_ref, hid_hbm, tab_ref, msk_hbm, kc_hbm, vc_hbm,
           wq_hbm, wk_hbm, wv_hbm, wo_hbm, wg_hbm, wu_hbm, wd_hbm, wr_ref, ag_ref, mg_ref, fg_ref,
           out_hbm, kn_ref, vn_ref,
           wqkv, wo, wg, wu, wd, h_buf, h_out, h_mid, rows_buf, msk_all,
           acc, pair_buf, c_send, c_own, c_recv, kbuf, vbuf, cs_s, q_ht, o_ht, o_s, act_s, col_s,
           w_sem, we_sem, hin_sem, kv_sem, own_sem, msk_send, msk_recv,
           ag_send, ag_recv, rl_send, rl_recv, fw_send, fw_recv, pr_send, pr_recv, cs_send, cs_recv,
           h_send, h_recv, f_send, f_recv, f_loc):
    steps, rows, width, ep_size, pp_size, heads, kv_heads, head, ctx, toks, local_e = cfg
    chips = ep_size // 2
    dp_i, stage, me = lax.axis_index("dp"), lax.axis_index("pp"), lax.axis_index("ep")
    core = lax.rem(me, 2)
    chip = me // 2
    partner = me + 1 - 2 * core

    def same_core(dx):
        return 2 * lax.rem(chip + dx, chips) + core

    last = pp_size - 1
    micros = rows // toks
    kvw = kv_heads * head
    qw = heads * head
    rep_n = heads // kv_heads
    hrows = toks * heads
    chunks = width // CHUNK
    assert chips == 4
    right, far, left = same_core(1), same_core(2), same_core(3)

    def place(idx):
        return lax.rem(idx, 2) * chips + idx // 2

    def ep_id(idx):
        return (dp_i, stage, idx)

    barrier = pltpu.get_barrier_semaphore()
    for d in range(1, ep_size):
        pl.semaphore_signal(barrier, inc=1, device_id=ep_id(lax.rem(me + d, ep_size)), device_id_type=MESH)
    for d in range(1, pp_size):
        pl.semaphore_signal(barrier, inc=1, device_id=(dp_i, lax.rem(stage + d, pp_size), me), device_id_type=MESH)

    def wcopies():
        return [pltpu.make_async_copy(wq_hbm, wqkv.at[:, pl.ds(0, qw)], w_sem.at[0]),
                pltpu.make_async_copy(wk_hbm, wqkv.at[:, pl.ds(qw, kvw)], w_sem.at[1]),
                pltpu.make_async_copy(wv_hbm, wqkv.at[:, pl.ds(qw + kvw, kvw)], w_sem.at[2]),
                pltpu.make_async_copy(wo_hbm, wo, w_sem.at[3])]

    def ecopies(e):
        return [pltpu.make_async_copy(wg_hbm.at[e], wg.at[e], we_sem.at[0, e]),
                pltpu.make_async_copy(wu_hbm.at[e], wu.at[e], we_sem.at[1, e]),
                pltpu.make_async_copy(wd_hbm.at[e], wd.at[e], we_sem.at[2, e])]

    def kv_copies(i, slot):
        return [pltpu.make_async_copy(kc_hbm.at[i], kbuf.at[slot], kv_sem.at[0, slot]),
                pltpu.make_async_copy(vc_hbm.at[i], vbuf.at[slot], kv_sem.at[1, slot])]

    hin = pltpu.make_async_copy(hid_hbm, h_buf, hin_sem)
    own_msk = pltpu.make_async_copy(msk_hbm, msk_all.at[place(me)], own_sem)

    @pl.when(stage == 0)
    def _():
        hin.start()

    wc = wcopies()
    wc[0].start()
    wc[1].start()
    wc[2].start()
    for cp in kv_copies(0, 0):
        cp.start()
    wc[3].start()
    own_msk.start()
    pl.semaphore_wait(barrier, ep_size - 1 + pp_size - 1)

    def msk_copy(d):
        return pltpu.make_async_remote_copy(
            src_ref=msk_hbm, dst_ref=msk_all.at[place(me)], send_sem=msk_send.at[d], recv_sem=msk_recv.at[d],
            device_id=ep_id(lax.rem(me + d, ep_size)), device_id_type=MESH)

    for d in range(1, ep_size):
        msk_copy(d).start()

    def ag_copy(j, way):
        slot = lax.rem(j, SLOTS)
        return pltpu.make_async_remote_copy(
            src_ref=rows_buf.at[slot, place(me)], dst_ref=rows_buf.at[slot, place(me)],
            send_sem=ag_send.at[slot, way], recv_sem=ag_recv.at[slot, way],
            device_id=ep_id((partner, right, left)[way]), device_id_type=MESH)

    def relay_copy(j, way):
        slot = lax.rem(j, SLOTS)
        src = place((left, right)[way - 1])
        part = pl.ds((way - 1) * (rows // 2), rows // 2)
        return pltpu.make_async_remote_copy(
            src_ref=rows_buf.at[slot, src, part], dst_ref=rows_buf.at[slot, src, part],
            send_sem=rl_send.at[slot, way - 1], recv_sem=rl_recv.at[slot, way - 1],
            device_id=ep_id((right, left)[way - 1]), device_id_type=MESH)

    def fw_copy(j, way):
        slot = lax.rem(j, SLOTS)
        src = place((left, right, far)[way])
        return pltpu.make_async_remote_copy(
            src_ref=rows_buf.at[slot, src], dst_ref=rows_buf.at[slot, src],
            send_sem=fw_send.at[slot, way], recv_sem=fw_recv.at[slot, way],
            device_id=ep_id(partner), device_id_type=MESH)

    def pair_copy(j, n):
        slot = lax.rem(j, 2)
        return pltpu.make_async_remote_copy(
            src_ref=acc.at[n, 1 - core], dst_ref=pair_buf.at[slot, n],
            send_sem=pr_send.at[n], recv_sem=pr_recv.at[slot, n],
            device_id=ep_id(partner), device_id_type=MESH)

    def c_copy(j, n, kind):
        slot = lax.rem(j, SLOTS)
        half = lax.rem(j, 2)
        ahead, behind = (right, left) if n % 2 == 0 else (left, right)
        return pltpu.make_async_remote_copy(
            src_ref=c_send.at[half, kind, n], dst_ref=c_recv.at[slot, kind, n],
            send_sem=cs_send.at[half, kind, n], recv_sem=cs_recv.at[slot, kind, n],
            device_id=ep_id(behind if kind == 1 else ahead), device_id_type=MESH)

    def h_copy(j):
        return pltpu.make_async_remote_copy(
            src_ref=h_out.at[j], dst_ref=h_buf.at[j], send_sem=h_send.at[j], recv_sem=h_recv.at[j],
            device_id=(dp_i, lax.rem(stage + 1, pp_size), me), device_id_type=MESH)

    def f_copy(j, d):
        return pltpu.make_async_remote_copy(
            src_ref=h_out.at[j], dst_ref=out_hbm.at[j], send_sem=f_send.at[j, d - 1], recv_sem=f_recv.at[j],
            device_id=(dp_i, lax.rem(stage + d, pp_size), me), device_id_type=MESH)

    def f_local(j):
        return pltpu.make_async_copy(h_out.at[j], out_hbm.at[j], f_loc.at[j])

    lane_r = lax.broadcasted_iota(jnp.int32, (rows, 128), 1)
    low_half = lane_r % head < head // 2
    tk = ctx * kv_heads
    hrow = lax.broadcasted_iota(jnp.int32, (heads, tk), 0)
    hcol = lax.broadcasted_iota(jnp.int32, (heads, tk), 1)
    same_kv = hrow % kv_heads == hcol % kv_heads
    col_ctx = jnp.where(same_kv, hcol // kv_heads, ctx)
    scale = head ** -0.5

    def head_row(hh):
        return (hh % rep_n * kv_heads + hh // rep_n) * toks

    head_chunks = range(max(chunks - PART, 0))
    tail_chunks = range(max(chunks - PART, 0), chunks)

    def attn_proj(i):
        kslot = lax.rem(i, 2)

        @pl.when(i + 1 < steps)
        def _():
            for cp in kv_copies(i + 1, 1 - kslot):
                cp.start()

        @pl.when(i == 0)
        def _():
            wc[0].wait()
            wc[1].wait()
            wc[2].wait()
            for e in range(local_e):
                for cp in ecopies(e):
                    cp.start()

        @pl.when((i == 0) & (stage == 0))
        def _():
            hin.wait()

        @pl.when(stage > 0)
        def _():
            h_copy(i).wait_recv()

        hid = h_buf[i].astype(F32)
        normed = rms(hid, ag_ref[...].astype(F32))
        for m in range(micros):
            for t in range(toks):
                angle = tab_ref[pos_ref[t, i * micros + m]]
                cs_s[:, m * toks + t, :] = angle
        cos = cs_s[0]
        sin = cs_s[1]
        span = 512
        for n in range((qw + 2 * kvw) // span):
            blk = mm(normed, wqkv[:, n * span:(n + 1) * span]).astype(BF16).astype(F32)
            for b in range(span // 128):
                at = n * span + b * 128
                piece = blk[:, b * 128:(b + 1) * 128]
                if at < qw + kvw:
                    swap = jnp.where(low_half, pltpu.roll(piece, 128 - head // 2, 1), pltpu.roll(piece, head // 2, 1))
                    piece = piece * cos + swap * sin
                piece16 = piece.astype(BF16)
                piece = piece16.astype(F32)
                for p in range(128 // head):
                    hh = at // head + p
                    base = head_row(hh) if at < qw else hh * toks
                    for m in range(micros):
                        q_ht[m, base:base + toks, :] = piece[m * toks:(m + 1) * toks, p * head:(p + 1) * head]

    def attn_core(i):
        kslot = lax.rem(i, 2)
        for cp in kv_copies(i, kslot):
            cp.wait()
        for m in range(micros):
            own, vals, scores = [], [], []
            for c in range(toks // 2):
                q2 = []
                for t in (2 * c, 2 * c + 1):
                    q_t = q_ht[m, pl.ds(t, heads, stride=toks), :]
                    k_t = q_ht[m, pl.ds(hrows + t, kv_heads, stride=toks), :]
                    v_t = q_ht[m, pl.ds(hrows + kv_heads * toks + t, kv_heads, stride=toks), :]
                    kn_ref[i, m * toks + t] = k_t.astype(BF16)
                    vn_ref[i, m * toks + t] = v_t.astype(BF16)
                    own.append(jnp.sum(q_t * jnp.concatenate([k_t] * rep_n, axis=0), axis=-1, keepdims=True))
                    vals.append(jnp.concatenate([v_t] * rep_n, axis=0))
                    q2.append(q_t)
                at = (m * toks + 2 * c) * tk
                kt = kbuf[kslot, at:at + 2 * tk, :]
                both = lax.dot_general(jnp.concatenate(q2, axis=0).astype(BF16), kt, (((1,), (1,)), ((), ())), preferred_element_type=F32)
                scores += [both[0:heads, 0:tk], both[heads:, tk:]]
            masks = [col_ctx < pos_ref[t, i * micros + m] for t in range(toks)]
            scores = [jnp.where(masks[t], scores[t] * scale, -jnp.inf) for t in range(toks)]
            own = [o * scale for o in own]
            tops = [jnp.maximum(jnp.max(scores[t], axis=-1, keepdims=True), own[t]) for t in range(toks)]
            ws = [jnp.exp(scores[t] - tops[t]) for t in range(toks)]
            own_w = [jnp.exp(own[t] - tops[t]) for t in range(toks)]
            inv = [1.0 / (jnp.sum(ws[t], axis=-1, keepdims=True) + own_w[t]) for t in range(toks)]
            ws = [(ws[t] * inv[t]).astype(BF16) for t in range(toks)]
            own_w = [(own_w[t] * inv[t]).astype(BF16).astype(F32) for t in range(toks)]
            zero = jnp.zeros((heads, tk), BF16)
            for c in range(toks // 2):
                at = (m * toks + 2 * c) * tk
                vt = vbuf[kslot, at:at + 2 * tk, :]
                w2 = jnp.concatenate([jnp.concatenate([ws[2 * c], zero], axis=1), jnp.concatenate([zero, ws[2 * c + 1]], axis=1)], axis=0)
                o2 = mm(w2, vt)
                for u in range(2):
                    t = 2 * c + u
                    o_ht[m, pl.ds(t, heads, stride=toks), :] = o2[u * heads:(u + 1) * heads] + own_w[t] * vals[t]
            for b in range(qw // 128):
                pieces = []
                for p in range(128 // head):
                    base = head_row(b * (128 // head) + p)
                    pieces.append(o_ht[m, base:base + toks, :])
                o_s[m * toks:(m + 1) * toks, b * 128:(b + 1) * 128] = jnp.concatenate(pieces, axis=1).astype(BF16)

    def attn_out(i):
        span = 512

        @pl.when(i == 0)
        def _():
            wc[3].wait()

        mslot = lax.rem(i, SLOTS)
        attn = o_s[...]
        for n in range(width // span):
            part = mm(attn, wo[:, n * span:(n + 1) * span])
            h_mid[mslot, :, n * span:(n + 1) * span] = (h_buf[i, :, n * span:(n + 1) * span].astype(F32) + part).astype(BF16)
        rows_buf[mslot, place(me)] = rms(h_mid[mslot].astype(F32), mg_ref[...].astype(F32))
        for way in (1, 2, 0):
            ag_copy(i, way).start()

    def relay(i):
        for way in (1, 2):
            ag_copy(i, way).wait_recv()
            relay_copy(i, way).start()
            fw_copy(i, way - 1).start()

    def relay_far(i):
        for way in (1, 2):
            relay_copy(i, way).wait_recv()
        fw_copy(i, 2).start()

    def experts_up(j):
        slot = lax.rem(j, SLOTS)
        ag_copy(j, 0).wait_recv()
        for way in range(3):
            fw_copy(j, way).wait_recv()

        @pl.when(j == 0)
        def _():
            own_msk.wait()
            for d in range(1, ep_size):
                msk_copy(d).wait_recv()
            for e in range(local_e):
                for cp in ecopies(e):
                    cp.wait()

        total = ep_size * rows
        xs = rows_buf[slot].reshape(total, width)
        experts = wr_ref.shape[0]
        logits = lax.dot_general(xs, wr_ref[...], (((1,), (1,)), ((), ())), preferred_element_type=F32)
        chosen = msk_all[:, j].reshape(total, 128)[:, :experts].astype(F32) > 0.5
        logits = jnp.where(chosen, logits, -jnp.inf)
        numer = jnp.exp(logits - jnp.max(logits, axis=-1, keepdims=True))
        gates = numer / jnp.sum(numer, axis=-1, keepdims=True)
        lane = lax.broadcasted_iota(jnp.int32, (total, experts), 1)
        ff = wg.shape[2]
        for e in range(local_e):
            col = jnp.sum(jnp.where(lane == me * local_e + e, gates, 0.0), axis=-1, keepdims=True)
            col_s[e] = jnp.broadcast_to(col, (total, 128))

        xs = rows_buf[slot].reshape(total, width)
        for e in range(local_e):
            for n in range(ff // 256):
                gate_h = mm(xs, wg[e, :, n * 256:(n + 1) * 256])
                up_h = mm(xs, wu[e, :, n * 256:(n + 1) * 256])
                act_s[e, :, n * 256:(n + 1) * 256] = (jax.nn.silu(gate_h) * up_h).astype(BF16)

    def pair_sum(j, n):
        pair_copy(j, n).wait()
        half = lax.rem(j, 2)
        ahead, behind = (1, 3) if n % 2 == 0 else (3, 1)

        def both(dx):
            x = lax.rem(chip + dx, chips)
            return acc[n, core, x] + pair_buf[half, n, x]

        c_send[half, 0, n] = both(2)
        c_copy(j, n, 0).start()
        c_send[half, 1, n] = both(behind)
        c_copy(j, n, 1).start()
        c_send[half, 2, n] = both(ahead)
        c_own[half, n] = both(0)

    def experts_down(j):
        slot = lax.rem(j, SLOTS)
        for way in range(3):
            ag_copy(j, way).wait_send()
            fw_copy(j, way).wait_send()
        for way in (1, 2):
            relay_copy(j, way).wait_send()
        for first in range(0, chunks, PART):
            group = range(first, min(first + PART, chunks))
            for n in group:
                for e in range(local_e):
                    part = mm(act_s[e], wd[e, :, n * CHUNK:(n + 1) * CHUNK])
                    col = jnp.concatenate([col_s[e]] * (CHUNK // 128), axis=1)
                    term = (col * part).astype(BF16).astype(F32).reshape(2, chips, rows, CHUNK)
                    acc[n] = term if e == 0 else acc[n] + term
            for n in group:
                pair_copy(j, n).start()
        for n in head_chunks:
            pair_sum(j, n)

    def pass_on(j, group):
        half = lax.rem(j, 2)
        slot = lax.rem(j, SLOTS)
        for n in group:
            c_copy(j, n, 0).wait_recv()
            c_send[half, 2, n] = c_send[half, 2, n] + c_recv[slot, 0, n]
            c_copy(j, n, 2).start()

    def finish(j):
        slot = lax.rem(j, SLOTS)
        half = lax.rem(j, 2)
        for n in range(chunks):
            c_copy(j, n, 0).wait_send()
            for kind in (1, 2):
                c_copy(j, n, kind).wait()
        parts = []
        for n in range(chunks):
            total = c_own[half, n]
            total = total + c_recv[slot, 1, n] + c_recv[slot, 2, n]
            parts.append((h_mid[slot, :, n * CHUNK:(n + 1) * CHUNK].astype(F32) + total.astype(BF16).astype(F32)).astype(BF16))
        hid = jnp.concatenate(parts, axis=1)

        @pl.when(stage < last)
        def _():
            h_out[j] = hid
            h_copy(j).start()

        @pl.when(stage == last)
        def _():
            h_out[j] = rms(hid.astype(F32), fg_ref[...].astype(F32))
            for d in range(1, pp_size):
                f_copy(j, d).start()
            f_local(j).start()

    def step(i, carry):
        fresh = i < steps
        middle = (i >= 1) & (i <= steps)
        old = i >= 2

        @pl.when(fresh)
        def _():
            attn_proj(i)

        @pl.when(old)
        def _():
            for n in tail_chunks:
                pair_sum(i - 2, n)

        @pl.when(fresh)
        def _():
            attn_core(i)

        @pl.when(old)
        def _():
            pass_on(i - 2, head_chunks)

        @pl.when(fresh)
        def _():
            attn_out(i)

        @pl.when(old)
        def _():
            pass_on(i - 2, tail_chunks)

        @pl.when(middle)
        def _():
            experts_up(i - 1)

        @pl.when(fresh)
        def _():
            relay(i)

        @pl.when(old)
        def _():
            finish(i - 2)

        @pl.when(middle)
        def _():
            experts_down(i - 1)

        @pl.when(fresh)
        def _():
            relay_far(i)

        return carry

    lax.fori_loop(0, steps + 2, step, 0)

    for d in range(1, ep_size):
        msk_copy(d).wait_send()

    def drain(j, carry):
        @pl.when(stage < last)
        def _():
            h_copy(j).wait_send()
            f_copy(j, 1).wait_recv()

        @pl.when(stage == last)
        def _():
            for d in range(1, pp_size):
                f_copy(j, d).wait_send()
            f_local(j).wait()

        return carry

    lax.fori_loop(0, steps, drain, 0)


def solution(mesh):
    ep_size = mesh.shape["ep"]
    pp_size = mesh.shape["pp"]
    rows_spec = ("dp", "ep")
    three_dim = P("pp", None, None)
    two_dim = P("pp", None)
    expert_spec = P("pp", "ep", None, None)
    cache_spec = P("pp", None, rows_spec, None, None, None)
    new_spec = P("pp", None, rows_spec, None, None)
    in_specs = (P(None, rows_spec, None), P(None, rows_spec), cache_spec, cache_spec, P("pp", None, rows_spec, None), three_dim, three_dim, three_dim, three_dim, two_dim, two_dim, three_dim, expert_spec, expert_spec, expert_spec, P(None))
    out_specs = (P(None, rows_spec, None), new_spec, new_spec)

    def device_fn(hidden_in, seq_pos, k_cache, v_cache, expert_ids, w_query, w_key, w_value, w_out, attn_gain, mlp_gain, w_router, w_gate, w_up, w_down, final_gain):
        assert w_query.shape[0] == 1
        micro_count, toks, width = hidden_in.shape
        ctx, kv_heads, head = k_cache.shape[3:]
        heads = w_query.shape[2] // head
        local_e, ff = w_gate.shape[1], w_gate.shape[3]
        kvw, qw = kv_heads * head, heads * head
        steps = micro_count // GROUP
        rows = GROUP * toks
        chips = ep_size // 2
        half = head // 2
        inv_freq = np.float32(THETA) ** (-np.arange(half, dtype=np.float32) / np.float32(half))
        ang = (np.arange(ctx + 1, dtype=np.float32)[:, None] * inv_freq).astype(np.float32)
        cos, sin = np.cos(ang), np.sin(ang)
        reps = 128 // head
        table = jnp.asarray(np.stack([np.concatenate([cos, cos] * reps, axis=-1), np.concatenate([-sin, sin] * reps, axis=-1)], axis=1), F32)
        ids = expert_ids[0].reshape(steps, rows, -1)
        chosen = jnp.any(ids[..., :, None] == jnp.arange(128, dtype=jnp.int32), axis=-2).astype(BF16)
        cache_rows = GROUP * toks * ctx * kv_heads
        hrows = toks * heads
        chunks = width // CHUNK
        cfg = (steps, rows, width, ep_size, pp_size, heads, kv_heads, head, ctx, toks, local_e)
        vm = pl.BlockSpec(memory_space=pltpu.VMEM)
        hb = pl.BlockSpec(memory_space=pl.ANY)
        dma = pltpu.SemaphoreType.DMA
        call = pl.pallas_call(
            functools.partial(kernel, cfg),
            out_shape=(jax.ShapeDtypeStruct((steps, rows, width), BF16),
                       jax.ShapeDtypeStruct((steps, rows, kv_heads, head), BF16),
                       jax.ShapeDtypeStruct((steps, rows, kv_heads, head), BF16)),
            in_specs=[pl.BlockSpec(memory_space=pltpu.SMEM), hb, vm, hb, hb, hb] + [hb] * 7 + [vm] * 4,
            out_specs=(hb, vm, vm),
            scratch_shapes=[
                pltpu.VMEM((width, qw + 2 * kvw), BF16), pltpu.VMEM((qw, width), BF16),
                pltpu.VMEM((local_e, width, ff), BF16), pltpu.VMEM((local_e, width, ff), BF16), pltpu.VMEM((local_e, ff, width), BF16),
                pltpu.VMEM((steps, rows, width), BF16), pltpu.VMEM((steps, rows, width), BF16), pltpu.VMEM((SLOTS, rows, width), BF16),
                pltpu.VMEM((SLOTS, ep_size, rows, width), BF16), pltpu.VMEM((ep_size, steps, rows, 128), BF16),
                pltpu.VMEM((chunks, 2, chips, rows, CHUNK), F32), pltpu.VMEM((2, chunks, chips, rows, CHUNK), F32),
                pltpu.VMEM((2, 3, chunks, rows, CHUNK), F32), pltpu.VMEM((2, chunks, rows, CHUNK), F32), pltpu.VMEM((SLOTS, 3, chunks, rows, CHUNK), F32),
                pltpu.VMEM((2, cache_rows, head), BF16), pltpu.VMEM((2, cache_rows, head), BF16),
                pltpu.VMEM((2, rows, 128), F32), pltpu.VMEM((GROUP, hrows + 2 * kv_heads * toks, head), F32), pltpu.VMEM((GROUP, hrows, head), F32), pltpu.VMEM((rows, qw), BF16),
                pltpu.VMEM((local_e, ep_size * rows, ff), BF16), pltpu.VMEM((local_e, ep_size * rows, 128), F32),
                dma((4,)), dma((3, local_e)), dma(()), dma((2, 2)), dma(()), dma((ep_size,)), dma((ep_size,)),
                dma((SLOTS, 3)), dma((SLOTS, 3)), dma((SLOTS, 2)), dma((SLOTS, 2)), dma((SLOTS, 3)), dma((SLOTS, 3)), dma((chunks,)), dma((2, chunks)), dma((2, 3, chunks)), dma((SLOTS, 3, chunks)),
                dma((steps,)), dma((steps,)), dma((steps, pp_size - 1)), dma((steps,)), dma((steps,)),
            ],
            compiler_params=pltpu.CompilerParams(collective_id=0, has_side_effects=True, vmem_limit_bytes=66 * 1000 * 1000),
        )
        out, k_new, v_new = call(
            seq_pos.T, hidden_in.reshape(steps, rows, width), table, chosen,
            k_cache.reshape(steps, cache_rows, head), v_cache.reshape(steps, cache_rows, head),
            w_query[0], w_key[0], w_value[0], w_out[0], w_gate[0], w_up[0], w_down[0], w_router[0].T,
            attn_gain, mlp_gain, final_gain.reshape(1, width))
        new_shape = (1, micro_count, toks, kv_heads, head)
        return out.reshape(micro_count, toks, width), k_new.reshape(new_shape), v_new.reshape(new_shape)

    return jax.shard_map(device_fn, mesh=mesh, in_specs=in_specs, out_specs=out_specs, check_vma=False)
```

```python
import functools

import jax
import numpy as np
import jax.numpy as jnp
from jax import lax
from jax.experimental import pallas as pl
from jax.experimental.pallas import tpu as pltpu
from jax.sharding import PartitionSpec as P

THETA = 1000000.0
EPS = 1e-05
GROUP = 2
SLOTS = 3
UP_FIRST = 2
PARTS = 2
CHUNK = 256
MESH = pl.DeviceIdType.MESH
BF16 = jnp.bfloat16
F32 = jnp.float32


def rms(vals_f32, gain_f32):
    inv_rms = lax.rsqrt(jnp.mean(vals_f32 * vals_f32, axis=-1, keepdims=True) + EPS)
    return (vals_f32 * inv_rms * gain_f32).astype(BF16)


def mm(a, b):
    return jnp.dot(a, b, preferred_element_type=F32)


def kernel(cfg, pos_ref, hid_hbm, tab_ref, msk_ref, kc_hbm, vc_hbm,
           wq_hbm, wk_hbm, wv_hbm, wo_hbm, wg_hbm, wu_hbm, wd_hbm, wr_ref, ag_ref, mg_ref, fg_ref,
           out_hbm, kn_hbm, vn_hbm,
           wqkv, wo, wg, wu, wd, h_buf, h_out, h_mid, rows_buf,
           acc, pair_buf, c_send, c_own, c_recv, kbuf, vbuf, new_s, cs_s, q_ht, o_ht, o_s, act_s, col_s,
           w_sem, we_sem, hin_sem, kv_sem, new_sem,
           ag_send, ag_recv, rl_send, rl_recv, fw_send, fw_recv, pr_send, pr_recv, cs_send, cs_recv,
           h_send, h_recv, f_send, f_recv, f_loc):
    steps, rows, width, ep_size, pp_size, heads, kv_heads, head, ctx, toks, local_e = cfg
    chips = ep_size // 2
    dp_i, stage, me = lax.axis_index("dp"), lax.axis_index("pp"), lax.axis_index("ep")
    core = lax.rem(me, 2)
    chip = me // 2
    partner = me + 1 - 2 * core

    def same_core(dx):
        return 2 * lax.rem(chip + dx, chips) + core

    last = pp_size - 1
    micros = rows // toks
    kvw = kv_heads * head
    qw = heads * head
    rep_n = heads // kv_heads
    hrows = toks * heads
    chunks = width // CHUNK
    assert chips == 4
    right, far, left = same_core(1), same_core(2), same_core(3)

    def place(idx):
        return lax.rem(idx, 2) * chips + idx // 2

    def ep_id(idx):
        return (dp_i, stage, idx)

    barrier = pltpu.get_barrier_semaphore()
    for d in range(1, ep_size):
        pl.semaphore_signal(barrier, inc=1, device_id=ep_id(lax.rem(me + d, ep_size)), device_id_type=MESH)
    for d in range(1, pp_size):
        pl.semaphore_signal(barrier, inc=1, device_id=(dp_i, lax.rem(stage + d, pp_size), me), device_id_type=MESH)

    def wcopies():
        return [pltpu.make_async_copy(wq_hbm, wqkv.at[:, pl.ds(0, qw)], w_sem.at[0]),
                pltpu.make_async_copy(wk_hbm, wqkv.at[:, pl.ds(qw, kvw)], w_sem.at[1]),
                pltpu.make_async_copy(wv_hbm, wqkv.at[:, pl.ds(qw + kvw, kvw)], w_sem.at[2]),
                pltpu.make_async_copy(wo_hbm, wo, w_sem.at[3])]

    def ecopies(e):
        return [pltpu.make_async_copy(wg_hbm.at[e], wg.at[e], we_sem.at[0, e]),
                pltpu.make_async_copy(wu_hbm.at[e], wu.at[e], we_sem.at[1, e]),
                pltpu.make_async_copy(wd_hbm.at[e], wd.at[e], we_sem.at[2, e])]

    def kv_copies(i, slot):
        return [pltpu.make_async_copy(kc_hbm.at[i], kbuf.at[slot], kv_sem.at[0, slot]),
                pltpu.make_async_copy(vc_hbm.at[i], vbuf.at[slot], kv_sem.at[1, slot])]

    def new_copies(i):
        slot = lax.rem(i, 2)
        return [pltpu.make_async_copy(new_s.at[0, slot], kn_hbm.at[i], new_sem.at[0, slot]),
                pltpu.make_async_copy(new_s.at[1, slot], vn_hbm.at[i], new_sem.at[1, slot])]

    hin = pltpu.make_async_copy(hid_hbm, h_buf, hin_sem)

    @pl.when(stage == 0)
    def _():
        hin.start()

    wc = wcopies()
    wc[0].start()
    wc[1].start()
    wc[2].start()
    for cp in kv_copies(0, 0):
        cp.start()
    wc[3].start()
    pl.semaphore_wait(barrier, ep_size - 1 + pp_size - 1)

    def half_rows(which):
        return pl.ds(which * (rows // 2), rows // 2)

    def ag_copy(j, way):
        slot = lax.rem(j, SLOTS)
        block = rows_buf.at[slot, place(me)]
        if way:
            block = rows_buf.at[slot, place(me), half_rows((0, 1, 1, 0)[way - 1])]
        return pltpu.make_async_remote_copy(
            src_ref=block, dst_ref=block,
            send_sem=ag_send.at[slot, way], recv_sem=ag_recv.at[slot, way],
            device_id=ep_id((partner, right, right, left, left)[way]), device_id_type=MESH)

    def relay_copy(j, way):
        slot = lax.rem(j, SLOTS)
        block = rows_buf.at[slot, place((left, right)[way - 1]), half_rows(way - 1)]
        return pltpu.make_async_remote_copy(
            src_ref=block, dst_ref=block,
            send_sem=rl_send.at[slot, way - 1], recv_sem=rl_recv.at[slot, way - 1],
            device_id=ep_id((right, left)[way - 1]), device_id_type=MESH)

    def fw_copy(j, way):
        slot = lax.rem(j, SLOTS)
        src = place((left, right, far)[way])
        return pltpu.make_async_remote_copy(
            src_ref=rows_buf.at[slot, src], dst_ref=rows_buf.at[slot, src],
            send_sem=fw_send.at[slot, way], recv_sem=fw_recv.at[slot, way],
            device_id=ep_id(partner), device_id_type=MESH)

    def pair_copy(j, p):
        slot = lax.rem(j, 2)
        return pltpu.make_async_remote_copy(
            src_ref=acc.at[p, 1 - core], dst_ref=pair_buf.at[slot, p],
            send_sem=pr_send.at[p], recv_sem=pr_recv.at[slot, p],
            device_id=ep_id(partner), device_id_type=MESH)

    def c_copy(j, p, kind, way):
        slot = lax.rem(j, SLOTS)
        half = lax.rem(j, 2)
        return pltpu.make_async_remote_copy(
            src_ref=c_send.at[half, kind, p, way], dst_ref=c_recv.at[slot, kind, p, way],
            send_sem=cs_send.at[half, kind, p, way], recv_sem=cs_recv.at[slot, kind, p, way],
            device_id=ep_id((right, left)[way]), device_id_type=MESH)

    def h_copy(j):
        return pltpu.make_async_remote_copy(
            src_ref=h_out.at[j], dst_ref=h_buf.at[j], send_sem=h_send.at[j], recv_sem=h_recv.at[j],
            device_id=(dp_i, lax.rem(stage + 1, pp_size), me), device_id_type=MESH)

    def f_copy(j, d):
        return pltpu.make_async_remote_copy(
            src_ref=h_out.at[j], dst_ref=out_hbm.at[j], send_sem=f_send.at[j, d - 1], recv_sem=f_recv.at[j],
            device_id=(dp_i, lax.rem(stage + d, pp_size), me), device_id_type=MESH)

    def f_local(j):
        return pltpu.make_async_copy(h_out.at[j], out_hbm.at[j], f_loc.at[j])

    lane_r = lax.broadcasted_iota(jnp.int32, (rows, 128), 1)
    low_half = lane_r % head < head // 2
    tk = ctx * kv_heads
    hrow = lax.broadcasted_iota(jnp.int32, (heads, tk), 0)
    hcol = lax.broadcasted_iota(jnp.int32, (heads, tk), 1)
    same_kv = hrow % kv_heads == hcol % kv_heads
    col_ctx = jnp.where(same_kv, hcol // kv_heads, ctx)
    scale = head ** -0.5

    def head_row(hh):
        return (hh % rep_n * kv_heads + hh // rep_n) * toks

    per = chunks // PARTS
    mid = rows // 2

    def attn_proj(i):
        kslot = lax.rem(i, 2)

        @pl.when(i + 1 < steps)
        def _():
            for cp in kv_copies(i + 1, 1 - kslot):
                cp.start()

        @pl.when(i == 0)
        def _():
            wc[0].wait()
            wc[1].wait()
            wc[2].wait()
            for e in range(local_e):
                for cp in ecopies(e):
                    cp.start()

        @pl.when((i == 0) & (stage == 0))
        def _():
            hin.wait()

        @pl.when(stage > 0)
        def _():
            h_copy(i).wait_recv()

        hid = h_buf[i].astype(F32)
        normed = rms(hid, ag_ref[...].astype(F32))
        for m in range(micros):
            for t in range(toks):
                angle = tab_ref[pos_ref[t, i * micros + m]]
                cs_s[:, m * toks + t, :] = angle
        cos = cs_s[0]
        sin = cs_s[1]
        span = 512
        for n in range((qw + 2 * kvw) // span):
            blk = mm(normed, wqkv[:, n * span:(n + 1) * span]).astype(BF16).astype(F32)
            for b in range(span // 128):
                at = n * span + b * 128
                piece = blk[:, b * 128:(b + 1) * 128]
                if at < qw + kvw:
                    swap = jnp.where(low_half, pltpu.roll(piece, 128 - head // 2, 1), pltpu.roll(piece, head // 2, 1))
                    piece = piece * cos + swap * sin
                piece16 = piece.astype(BF16)
                piece = piece16.astype(F32)
                for p in range(128 // head):
                    hh = at // head + p
                    base = head_row(hh) if at < qw else hh * toks
                    for m in range(micros):
                        q_ht[m, base:base + toks, :] = piece[m * toks:(m + 1) * toks, p * head:(p + 1) * head]

    def attn_core(i):
        kslot = lax.rem(i, 2)
        for cp in kv_copies(i, kslot):
            cp.wait()

        @pl.when(i >= 2)
        def _():
            for cp in new_copies(i - 2):
                cp.wait()

        for m in range(micros):
            own, vals, scores = [], [], []
            for c in range(toks // 2):
                q2 = []
                for t in (2 * c, 2 * c + 1):
                    q_t = q_ht[m, pl.ds(t, heads, stride=toks), :]
                    k_t = q_ht[m, pl.ds(hrows + t, kv_heads, stride=toks), :]
                    v_t = q_ht[m, pl.ds(hrows + kv_heads * toks + t, kv_heads, stride=toks), :]
                    new_s[0, kslot, m * toks + t] = k_t.astype(BF16)
                    new_s[1, kslot, m * toks + t] = v_t.astype(BF16)
                    own.append(jnp.sum(q_t * jnp.concatenate([k_t] * rep_n, axis=0), axis=-1, keepdims=True))
                    vals.append(jnp.concatenate([v_t] * rep_n, axis=0))
                    q2.append(q_t)
                at = (m * toks + 2 * c) * tk
                kt = kbuf[kslot, at:at + 2 * tk, :]
                both = lax.dot_general(jnp.concatenate(q2, axis=0).astype(BF16), kt, (((1,), (1,)), ((), ())), preferred_element_type=F32)
                scores += [both[0:heads, 0:tk], both[heads:, tk:]]
            masks = [col_ctx < pos_ref[t, i * micros + m] for t in range(toks)]
            scores = [jnp.where(masks[t], scores[t] * scale, -jnp.inf) for t in range(toks)]
            own = [o * scale for o in own]
            tops = [jnp.maximum(jnp.max(scores[t], axis=-1, keepdims=True), own[t]) for t in range(toks)]
            ws = [jnp.exp(scores[t] - tops[t]) for t in range(toks)]
            own_w = [jnp.exp(own[t] - tops[t]) for t in range(toks)]
            inv = [1.0 / (jnp.sum(ws[t], axis=-1, keepdims=True) + own_w[t]) for t in range(toks)]
            ws = [(ws[t] * inv[t]).astype(BF16) for t in range(toks)]
            own_w = [(own_w[t] * inv[t]).astype(BF16).astype(F32) for t in range(toks)]
            zero = jnp.zeros((heads, tk), BF16)
            for c in range(toks // 2):
                at = (m * toks + 2 * c) * tk
                vt = vbuf[kslot, at:at + 2 * tk, :]
                w2 = jnp.concatenate([jnp.concatenate([ws[2 * c], zero], axis=1), jnp.concatenate([zero, ws[2 * c + 1]], axis=1)], axis=0)
                o2 = mm(w2, vt)
                for u in range(2):
                    t = 2 * c + u
                    o_ht[m, pl.ds(t, heads, stride=toks), :] = o2[u * heads:(u + 1) * heads] + own_w[t] * vals[t]
            for b in range(qw // 128):
                pieces = []
                for p in range(128 // head):
                    base = head_row(b * (128 // head) + p)
                    pieces.append(o_ht[m, base:base + toks, :])
                o_s[m * toks:(m + 1) * toks, b * 128:(b + 1) * 128] = jnp.concatenate(pieces, axis=1).astype(BF16)

        for cp in new_copies(i):
            cp.start()

    def attn_out(i):
        span = 512

        @pl.when(i == 0)
        def _():
            wc[3].wait()

        mslot = lax.rem(i, SLOTS)
        attn = o_s[...]
        for n in range(width // span):
            part = mm(attn, wo[:, n * span:(n + 1) * span])
            h_mid[mslot, :, n * span:(n + 1) * span] = (h_buf[i, :, n * span:(n + 1) * span].astype(F32) + part).astype(BF16)
        rows_buf[mslot, place(me), :, 0:width] = rms(h_mid[mslot].astype(F32), mg_ref[...].astype(F32))
        rows_buf[mslot, place(me), :, width:width + 128] = msk_ref[i]

    def send_rows(i):
        for way in (1, 3, 2, 4, 0):
            ag_copy(i, way).start()

    def relay(i):
        for way in (1, 2):
            ag_copy(i, 2 * way - 1).wait_recv()
            relay_copy(i, way).start()

    def relay_near(i):
        for way in (1, 2):
            ag_copy(i, 2 * way).wait_recv()
            fw_copy(i, way - 1).start()

    def relay_far(i):
        for way in (1, 2):
            relay_copy(i, way).wait_recv()
        fw_copy(i, 2).start()

    def experts_up_first(j):
        slot = lax.rem(j, SLOTS)
        ag_copy(j, 0).wait_recv()
        for way in range(3):
            fw_copy(j, way).wait_recv()

        @pl.when(j == 0)
        def _():
            for e in range(local_e):
                for cp in ecopies(e):
                    cp.wait()

        total = ep_size * rows
        xs = rows_buf[slot, :, :, 0:width].reshape(total, width)
        experts = wr_ref.shape[0]
        logits = lax.dot_general(xs, wr_ref[...], (((1,), (1,)), ((), ())), preferred_element_type=F32)
        chosen = rows_buf[slot, :, :, width:width + 128].reshape(total, 128)[:, :experts].astype(F32) > 0.5
        logits = jnp.where(chosen, logits, -jnp.inf)
        numer = jnp.exp(logits - jnp.max(logits, axis=-1, keepdims=True))
        gates = numer / jnp.sum(numer, axis=-1, keepdims=True)
        lane = lax.broadcasted_iota(jnp.int32, (total, experts), 1)
        for e in range(local_e):
            col = jnp.sum(jnp.where(lane == me * local_e + e, gates, 0.0), axis=-1, keepdims=True)
            col_s[e] = jnp.broadcast_to(col, (total, 128))

        experts_up(j, range(UP_FIRST))

    def experts_up(j, group):
        slot = lax.rem(j, SLOTS)
        ff = wg.shape[2]
        xs = rows_buf[slot, :, :, 0:width].reshape(ep_size * rows, width)
        for e in group:
            for n in range(ff // 256):
                gate_h = mm(xs, wg[e, :, n * 256:(n + 1) * 256])
                up_h = mm(xs, wu[e, :, n * 256:(n + 1) * 256])
                act_s[e, :, n * 256:(n + 1) * 256] = (jax.nn.silu(gate_h) * up_h).astype(BF16)

    def pair_sum(j, p):
        half = lax.rem(j, 2)

        def both(dx, lo, hi):
            x = lax.rem(chip + dx, chips)
            return acc[p, core, :, x, lo:hi, :] + pair_buf[half, p, :, x, lo:hi, :]

        pair_copy(j, p).wait()
        c_send[half, 0, p, 0] = both(2, 0, mid)
        c_send[half, 0, p, 1] = both(2, mid, rows)
        for way in range(2):
            c_copy(j, p, 0, way).start()
        c_send[half, 1, p, 0] = both(1, mid, rows)
        c_send[half, 1, p, 1] = both(3, 0, mid)
        for way in range(2):
            c_copy(j, p, 1, way).start()
        c_send[half, 2, p, 0] = both(1, 0, mid)
        c_send[half, 2, p, 1] = both(3, mid, rows)
        c_own[half, p] = both(0, 0, rows)

    def sent_rows(j):
        for way in range(5):
            ag_copy(j, way).wait_send()
        for way in range(3):
            fw_copy(j, way).wait_send()
        for way in (1, 2):
            relay_copy(j, way).wait_send()

    def experts_down(j, p):
        for c in range(per):
            at = (p * per + c) * CHUNK
            for e in range(local_e):
                part = mm(act_s[e], wd[e, :, at:at + CHUNK])
                col = jnp.concatenate([col_s[e]] * (CHUNK // 128), axis=1)
                term = (col * part).astype(BF16).astype(F32).reshape(2, chips, rows, CHUNK)
                for k in range(2):
                    acc[p, k, c] = term[k] if e == 0 else acc[p, k, c] + term[k]
        pair_copy(j, p).start()

    def pass_on(j, p):
        half = lax.rem(j, 2)
        slot = lax.rem(j, SLOTS)
        for way in range(2):
            c_copy(j, p, 0, way).wait_recv()
            c_send[half, 2, p, way] = c_send[half, 2, p, way] + c_recv[slot, 0, p, way]
            c_copy(j, p, 2, way).start()

    def finish(j):
        slot = lax.rem(j, SLOTS)
        half = lax.rem(j, 2)
        for p in range(PARTS):
            for way in range(2):
                c_copy(j, p, 0, way).wait_send()
                c_copy(j, p, 1, way).wait()
                c_copy(j, p, 2, way).wait()
        parts = []
        for p in range(PARTS):
            for c in range(per):
                upper = c_recv[slot, 2, p, 0, c] + c_recv[slot, 1, p, 1, c]
                lower = c_recv[slot, 1, p, 0, c] + c_recv[slot, 2, p, 1, c]
                total = c_own[half, p, c] + jnp.concatenate([upper, lower], axis=0)
                at = (p * per + c) * CHUNK
                parts.append((h_mid[slot, :, at:at + CHUNK].astype(F32) + total.astype(BF16).astype(F32)).astype(BF16))
        hid = jnp.concatenate(parts, axis=1)

        @pl.when(stage < last)
        def _():
            h_out[j] = hid
            h_copy(j).start()

        @pl.when(stage == last)
        def _():
            h_out[j] = rms(hid.astype(F32), fg_ref[...].astype(F32).reshape(1, width))
            for d in range(1, pp_size):
                f_copy(j, d).start()
            f_local(j).start()

    def head_sum(j):
        pair_sum(j, 0)

    def tail_sum(j):
        pair_sum(j, 1)

    def head_on(j):
        pass_on(j, 0)

    def tail_on(j):
        pass_on(j, 1)

    def up_first(j):
        experts_up_first(j)

    def up_rest(j):
        experts_up(j, range(UP_FIRST, local_e))

    def down_head(j):
        sent_rows(j)
        experts_down(j, 0)

    def down_tail(j):
        experts_down(j, 1)

    order = (
        (attn_proj, 0),
        (relay_far, 1),
        (tail_sum, 2),
        (attn_core, 0),
        (attn_out, 0),
        (send_rows, 0),
        (head_on, 2),
        (up_first, 1),
        (tail_on, 2),
        (up_rest, 1),
        (relay, 0),
        (down_head, 1),
        (relay_near, 0),
        (finish, 2),
        (down_tail, 1),
        (head_sum, 1),
    )

    def step(i, carry):
        for phase, lag in order:
            @pl.when((i >= lag) & (i < steps + lag))
            def _(phase=phase, lag=lag):
                phase(i - lag)

        return carry

    lax.fori_loop(0, steps + max(lag for _, lag in order), step, 0)

    for i in range(max(steps - 2, 0), steps):
        for cp in new_copies(i):
            cp.wait()

    def drain(j, carry):
        @pl.when(stage < last)
        def _():
            h_copy(j).wait_send()
            f_copy(j, 1).wait_recv()

        @pl.when(stage == last)
        def _():
            for d in range(1, pp_size):
                f_copy(j, d).wait_send()
            f_local(j).wait()

        return carry

    lax.fori_loop(0, steps, drain, 0)


def copy_kernel(count, *refs):
    src, dst, buf, in_sem, out_sem = refs[:count], refs[count:2 * count], refs[2 * count:3 * count], refs[-2], refs[-1]
    ins = [pltpu.make_async_copy(src[n], buf[n], in_sem.at[n]) for n in range(count)]
    outs = [pltpu.make_async_copy(buf[n], dst[n], out_sem.at[n]) for n in range(count)]
    for cp in ins:
        cp.start()
    for n in range(count):
        ins[n].wait()
        outs[n].start()
    for cp in outs:
        cp.wait()


def solution(mesh):
    ep_size = mesh.shape["ep"]
    pp_size = mesh.shape["pp"]
    rows_spec = ("dp", "ep")
    three_dim = P("pp", None, None)
    two_dim = P("pp", None)
    expert_spec = P("pp", "ep", None, None)
    cache_spec = P("pp", None, rows_spec, None, None, None)
    new_spec = P("pp", None, rows_spec, None, None)
    in_specs = (P(None, rows_spec, None), P(None, rows_spec), cache_spec, cache_spec, P("pp", None, rows_spec, None), three_dim, three_dim, three_dim, three_dim, two_dim, two_dim, three_dim, expert_spec, expert_spec, expert_spec, P(None))
    out_specs = (P(None, rows_spec, None), new_spec, new_spec)

    def device_fn(hidden_in, seq_pos, k_cache, v_cache, expert_ids, w_query, w_key, w_value, w_out, attn_gain, mlp_gain, w_router, w_gate, w_up, w_down, final_gain):
        assert w_query.shape[0] == 1
        micro_count, toks, width = hidden_in.shape
        ctx, kv_heads, head = k_cache.shape[3:]
        heads = w_query.shape[2] // head
        local_e, ff = w_gate.shape[1], w_gate.shape[3]
        kvw, qw = kv_heads * head, heads * head
        steps = micro_count // GROUP
        rows = GROUP * toks
        chips = ep_size // 2
        half = head // 2
        inv_freq = np.float32(THETA) ** (-np.arange(half, dtype=np.float32) / np.float32(half))
        ang = (np.arange(ctx + 1, dtype=np.float32)[:, None] * inv_freq).astype(np.float32)
        cos, sin = np.cos(ang), np.sin(ang)
        reps = 128 // head
        table = jnp.asarray(np.stack([np.concatenate([cos, cos] * reps, axis=-1), np.concatenate([-sin, sin] * reps, axis=-1)], axis=1), F32)
        ids = expert_ids[0].reshape(steps, rows, -1)
        chosen = jnp.max((ids[..., :, None] == jnp.arange(128, dtype=jnp.int32)).astype(BF16), axis=-2)
        cache_rows = GROUP * toks * ctx * kv_heads
        hrows = toks * heads
        per = width // CHUNK // PARTS
        cfg = (steps, rows, width, ep_size, pp_size, heads, kv_heads, head, ctx, toks, local_e)
        vm = pl.BlockSpec(memory_space=pltpu.VMEM)
        hb = pl.BlockSpec(memory_space=pl.ANY)
        dma = pltpu.SemaphoreType.DMA
        call = pl.pallas_call(
            functools.partial(kernel, cfg),
            out_shape=(jax.ShapeDtypeStruct((steps, rows, width), BF16),
                       jax.ShapeDtypeStruct((steps, rows, kv_heads, head), BF16),
                       jax.ShapeDtypeStruct((steps, rows, kv_heads, head), BF16)),
            in_specs=[pl.BlockSpec(memory_space=pltpu.SMEM), hb, vm, vm, hb, hb] + [hb] * 7 + [vm] * 4,
            out_specs=(hb, hb, hb),
            scratch_shapes=[
                pltpu.VMEM((width, qw + 2 * kvw), BF16), pltpu.VMEM((qw, width), BF16),
                pltpu.VMEM((local_e, width, ff), BF16), pltpu.VMEM((local_e, width, ff), BF16), pltpu.VMEM((local_e, ff, width), BF16),
                pltpu.VMEM((steps, rows, width), BF16), pltpu.VMEM((steps, rows, width), BF16), pltpu.VMEM((SLOTS, rows, width), BF16),
                pltpu.VMEM((SLOTS, ep_size, rows, width + 128), BF16),
                pltpu.VMEM((PARTS, 2, per, chips, rows, CHUNK), F32), pltpu.VMEM((2, PARTS, per, chips, rows, CHUNK), F32),
                pltpu.VMEM((2, 3, PARTS, 2, per, rows // 2, CHUNK), F32), pltpu.VMEM((2, PARTS, per, rows, CHUNK), F32), pltpu.VMEM((SLOTS, 3, PARTS, 2, per, rows // 2, CHUNK), F32),
                pltpu.VMEM((2, cache_rows, head), BF16), pltpu.VMEM((2, cache_rows, head), BF16),
                pltpu.VMEM((2, 2, rows, kv_heads, head), BF16), pltpu.VMEM((2, rows, 128), F32), pltpu.VMEM((GROUP, hrows + 2 * kv_heads * toks, head), F32), pltpu.VMEM((GROUP, hrows, head), F32), pltpu.VMEM((rows, qw), BF16),
                pltpu.VMEM((local_e, ep_size * rows, ff), BF16), pltpu.VMEM((local_e, ep_size * rows, 128), F32),
                dma((4,)), dma((3, local_e)), dma(()), dma((2, 2)), dma((2, 2)),
                dma((SLOTS, 5)), dma((SLOTS, 5)), dma((SLOTS, 2)), dma((SLOTS, 2)), dma((SLOTS, 3)), dma((SLOTS, 3)), dma((PARTS,)), dma((2, PARTS)), dma((2, 3, PARTS, 2)), dma((SLOTS, 3, PARTS, 2)),
                dma((steps,)), dma((steps,)), dma((steps, pp_size - 1)), dma((steps,)), dma((steps,)),
            ],
            compiler_params=pltpu.CompilerParams(collective_id=0, has_side_effects=True, vmem_limit_bytes=66 * 1000 * 1000),
        )
        out, k_new, v_new = call(
            seq_pos.T, hidden_in.reshape(steps, rows, width), table, chosen,
            k_cache.reshape(steps, cache_rows, head), v_cache.reshape(steps, cache_rows, head),
            w_query[0], w_key[0], w_value[0], w_out[0], w_gate[0], w_up[0], w_down[0], w_router[0].T,
            attn_gain, mlp_gain, final_gain)
        results = (out, k_new, v_new)
        out, k_new, v_new = pl.pallas_call(
            functools.partial(copy_kernel, len(results)),
            out_shape=[jax.ShapeDtypeStruct(r.shape, r.dtype) for r in results],
            in_specs=[hb] * len(results), out_specs=[hb] * len(results),
            scratch_shapes=[pltpu.VMEM(r.shape, r.dtype) for r in results] + [dma((len(results),))] * 2,
        )(*results)
        new_shape = (1, micro_count, toks, kv_heads, head)
        return out.reshape(micro_count, toks, width), k_new.reshape(new_shape), v_new.reshape(new_shape)

    return jax.shard_map(device_fn, mesh=mesh, in_specs=in_specs, out_specs=out_specs, check_vma=False)
```

```python
import functools

import jax
import numpy as np
import jax.numpy as jnp
from jax import lax
from jax.experimental import pallas as pl
from jax.experimental.pallas import tpu as pltpu
from jax.sharding import PartitionSpec as P

THETA = 1000000.0
EPS = 1e-05
GROUP = 2
SLOTS = 3
UP_FIRST = 2
PARTS = 2
CHUNK = 256
MESH = pl.DeviceIdType.MESH
BF16 = jnp.bfloat16
F32 = jnp.float32


def rms(vals_f32, gain_f32):
    inv_rms = lax.rsqrt(jnp.mean(vals_f32 * vals_f32, axis=-1, keepdims=True) + EPS)
    return (vals_f32 * inv_rms * gain_f32).astype(BF16)


def mm(a, b):
    return jnp.dot(a, b, preferred_element_type=F32)


def kernel(cfg, pos_ref, hid_hbm, tab_ref, msk_ref, kc_hbm, vc_hbm,
           wq_hbm, wk_hbm, wv_hbm, wo_hbm, wg_hbm, wu_hbm, wd_hbm, wr_ref, ag_ref, mg_ref, fg_ref,
           out_hbm, kn_hbm, vn_hbm,
           wqkv, wo, wg, wu, wd, h_buf, h_out, h_mid, rows_buf,
           acc, pair_buf, c_send, c_own, c_recv, kbuf, vbuf, new_s, cs_s, q_ht, o_ht, o_s, act_s, col_s,
           w_sem, we_sem, hin_sem, kv_sem, new_sem,
           ag_send, ag_recv, rl_send, rl_recv, fw_send, fw_recv, pr_send, pr_recv, cs_send, cs_recv,
           h_send, h_recv, f_send, f_recv, f_loc):
    steps, rows, width, ep_size, pp_size, heads, kv_heads, head, ctx, toks, local_e = cfg
    chips = ep_size // 2
    dp_i, stage, me = lax.axis_index("dp"), lax.axis_index("pp"), lax.axis_index("ep")
    core = lax.rem(me, 2)
    chip = me // 2
    partner = me + 1 - 2 * core

    def same_core(dx):
        return 2 * lax.rem(chip + dx, chips) + core

    last = pp_size - 1
    micros = rows // toks
    kvw = kv_heads * head
    qw = heads * head
    rep_n = heads // kv_heads
    hrows = toks * heads
    chunks = width // CHUNK
    assert chips == 4
    right, far, left = same_core(1), same_core(2), same_core(3)

    def place(idx):
        return lax.rem(idx, 2) * chips + idx // 2

    def ep_id(idx):
        return (dp_i, stage, idx)

    barrier = pltpu.get_barrier_semaphore()
    for d in range(1, ep_size):
        pl.semaphore_signal(barrier, inc=1, device_id=ep_id(lax.rem(me + d, ep_size)), device_id_type=MESH)
    for d in range(1, pp_size):
        pl.semaphore_signal(barrier, inc=1, device_id=(dp_i, lax.rem(stage + d, pp_size), me), device_id_type=MESH)

    def wcopies():
        return [pltpu.make_async_copy(wq_hbm, wqkv.at[:, pl.ds(0, qw)], w_sem.at[0]),
                pltpu.make_async_copy(wk_hbm, wqkv.at[:, pl.ds(qw, kvw)], w_sem.at[1]),
                pltpu.make_async_copy(wv_hbm, wqkv.at[:, pl.ds(qw + kvw, kvw)], w_sem.at[2]),
                pltpu.make_async_copy(wo_hbm, wo, w_sem.at[3])]

    def ecopies(e):
        return [pltpu.make_async_copy(wg_hbm.at[e], wg.at[e], we_sem.at[0, e]),
                pltpu.make_async_copy(wu_hbm.at[e], wu.at[e], we_sem.at[1, e]),
                pltpu.make_async_copy(wd_hbm.at[e], wd.at[e], we_sem.at[2, e])]

    def kv_copies(i, slot):
        return [pltpu.make_async_copy(kc_hbm.at[i], kbuf.at[slot], kv_sem.at[0, slot]),
                pltpu.make_async_copy(vc_hbm.at[i], vbuf.at[slot], kv_sem.at[1, slot])]

    def new_copies(i):
        slot = lax.rem(i, 2)
        return [pltpu.make_async_copy(new_s.at[0, slot], kn_hbm.at[i], new_sem.at[0, slot]),
                pltpu.make_async_copy(new_s.at[1, slot], vn_hbm.at[i], new_sem.at[1, slot])]

    hin = pltpu.make_async_copy(hid_hbm, h_buf, hin_sem)

    @pl.when(stage == 0)
    def _():
        hin.start()

    wc = wcopies()
    wc[0].start()
    wc[1].start()
    wc[2].start()
    for cp in kv_copies(0, 0):
        cp.start()
    wc[3].start()
    pl.semaphore_wait(barrier, ep_size - 1 + pp_size - 1)

    def half_rows(which):
        return pl.ds(which * (rows // 2), rows // 2)

    def ag_copy(j, way):
        slot = lax.rem(j, SLOTS)
        block = rows_buf.at[slot, place(me)]
        if way:
            block = rows_buf.at[slot, place(me), half_rows((0, 1, 1, 0)[way - 1])]
        return pltpu.make_async_remote_copy(
            src_ref=block, dst_ref=block,
            send_sem=ag_send.at[slot, way], recv_sem=ag_recv.at[slot, way],
            device_id=ep_id((partner, right, right, left, left)[way]), device_id_type=MESH)

    def relay_copy(j, way):
        slot = lax.rem(j, SLOTS)
        block = rows_buf.at[slot, place((left, right)[way - 1]), half_rows(way - 1)]
        return pltpu.make_async_remote_copy(
            src_ref=block, dst_ref=block,
            send_sem=rl_send.at[slot, way - 1], recv_sem=rl_recv.at[slot, way - 1],
            device_id=ep_id((right, left)[way - 1]), device_id_type=MESH)

    def fw_copy(j, way):
        slot = lax.rem(j, SLOTS)
        src = place((left, right, far)[way])
        return pltpu.make_async_remote_copy(
            src_ref=rows_buf.at[slot, src], dst_ref=rows_buf.at[slot, src],
            send_sem=fw_send.at[slot, way], recv_sem=fw_recv.at[slot, way],
            device_id=ep_id(partner), device_id_type=MESH)

    def pair_copy(j, p):
        slot = lax.rem(j, 2)
        return pltpu.make_async_remote_copy(
            src_ref=acc.at[p, 1 - core], dst_ref=pair_buf.at[slot, p],
            send_sem=pr_send.at[p], recv_sem=pr_recv.at[slot, p],
            device_id=ep_id(partner), device_id_type=MESH)

    def c_copy(j, p, kind, way):
        slot = lax.rem(j, SLOTS)
        half = lax.rem(j, 2)
        return pltpu.make_async_remote_copy(
            src_ref=c_send.at[half, kind, p, way], dst_ref=c_recv.at[slot, kind, p, way],
            send_sem=cs_send.at[half, kind, p, way], recv_sem=cs_recv.at[slot, kind, p, way],
            device_id=ep_id((right, left)[way]), device_id_type=MESH)

    def h_copy(j):
        return pltpu.make_async_remote_copy(
            src_ref=h_out.at[j], dst_ref=h_buf.at[j], send_sem=h_send.at[j], recv_sem=h_recv.at[j],
            device_id=(dp_i, lax.rem(stage + 1, pp_size), me), device_id_type=MESH)

    def f_copy(j, d):
        return pltpu.make_async_remote_copy(
            src_ref=h_out.at[j], dst_ref=out_hbm.at[j], send_sem=f_send.at[j, d - 1], recv_sem=f_recv.at[j],
            device_id=(dp_i, lax.rem(stage + d, pp_size), me), device_id_type=MESH)

    def f_local(j):
        return pltpu.make_async_copy(h_out.at[j], out_hbm.at[j], f_loc.at[j])

    lane_r = lax.broadcasted_iota(jnp.int32, (rows, 128), 1)
    low_half = lane_r % head < head // 2
    tk = ctx * kv_heads
    hrow = lax.broadcasted_iota(jnp.int32, (heads, tk), 0)
    hcol = lax.broadcasted_iota(jnp.int32, (heads, tk), 1)
    same_kv = hrow % kv_heads == hcol % kv_heads
    col_ctx = jnp.where(same_kv, hcol // kv_heads, ctx)
    scale = head ** -0.5

    def head_row(hh):
        return (hh % rep_n * kv_heads + hh // rep_n) * toks

    per = chunks // PARTS
    mid = rows // 2

    def attn_proj(i):
        kslot = lax.rem(i, 2)

        @pl.when(i + 1 < steps)
        def _():
            for cp in kv_copies(i + 1, 1 - kslot):
                cp.start()

        @pl.when(i == 0)
        def _():
            wc[0].wait()
            wc[1].wait()
            wc[2].wait()
            for e in range(local_e):
                for cp in ecopies(e):
                    cp.start()

        @pl.when((i == 0) & (stage == 0))
        def _():
            hin.wait()

        @pl.when(stage > 0)
        def _():
            h_copy(i).wait_recv()

        hid = h_buf[i].astype(F32)
        normed = rms(hid, ag_ref[...].astype(F32))
        for m in range(micros):
            for t in range(toks):
                angle = tab_ref[pos_ref[t, i * micros + m]]
                cs_s[:, m * toks + t, :] = angle
        cos = cs_s[0]
        sin = cs_s[1]
        span = 512
        for n in range((qw + 2 * kvw) // span):
            blk = mm(normed, wqkv[:, n * span:(n + 1) * span]).astype(BF16).astype(F32)
            for b in range(span // 128):
                at = n * span + b * 128
                piece = blk[:, b * 128:(b + 1) * 128]
                if at < qw + kvw:
                    swap = jnp.where(low_half, pltpu.roll(piece, 128 - head // 2, 1), pltpu.roll(piece, head // 2, 1))
                    piece = piece * cos + swap * sin
                piece16 = piece.astype(BF16)
                piece = piece16.astype(F32)
                for p in range(128 // head):
                    hh = at // head + p
                    base = head_row(hh) if at < qw else hh * toks
                    for m in range(micros):
                        q_ht[m, base:base + toks, :] = piece[m * toks:(m + 1) * toks, p * head:(p + 1) * head]

    def attn_core(i):
        kslot = lax.rem(i, 2)
        for cp in kv_copies(i, kslot):
            cp.wait()

        @pl.when(i == 0)
        def _():
            wc[3].wait()

        @pl.when(i >= 2)
        def _():
            for cp in new_copies(i - 2):
                cp.wait()

        own, vals, scores = [], [], []
        for m in range(micros):
            for c in range(toks // 2):
                q2 = []
                for t in (2 * c, 2 * c + 1):
                    q_t = q_ht[m, pl.ds(t, heads, stride=toks), :]
                    k_t = q_ht[m, pl.ds(hrows + t, kv_heads, stride=toks), :]
                    v_t = q_ht[m, pl.ds(hrows + kv_heads * toks + t, kv_heads, stride=toks), :]
                    new_s[0, kslot, m * toks + t] = k_t.astype(BF16)
                    new_s[1, kslot, m * toks + t] = v_t.astype(BF16)
                    own.append(jnp.sum(q_t * jnp.concatenate([k_t] * rep_n, axis=0), axis=-1, keepdims=True))
                    vals.append(jnp.concatenate([v_t] * rep_n, axis=0))
                    q2.append(q_t)
                at = (m * toks + 2 * c) * tk
                kt = kbuf[kslot, at:at + 2 * tk, :]
                both = lax.dot_general(jnp.concatenate(q2, axis=0).astype(BF16), kt, (((1,), (1,)), ((), ())), preferred_element_type=F32)
                scores += [both[0:heads, 0:tk], both[heads:, tk:]]
        every = range(micros * toks)
        masks = [col_ctx < pos_ref[n % toks, i * micros + n // toks] for n in every]
        scores = [jnp.where(masks[n], scores[n] * scale, -jnp.inf) for n in every]
        own = [o * scale for o in own]
        tops = [jnp.maximum(jnp.max(scores[n], axis=-1, keepdims=True), own[n]) for n in every]
        ws = [jnp.exp(scores[n] - tops[n]) for n in every]
        own_w = [jnp.exp(own[n] - tops[n]) for n in every]
        inv = [1.0 / (jnp.sum(ws[n], axis=-1, keepdims=True) + own_w[n]) for n in every]
        ws = [(ws[n] * inv[n]).astype(BF16) for n in every]
        own_w = [(own_w[n] * inv[n]).astype(BF16).astype(F32) for n in every]
        zero = jnp.zeros((heads, tk), BF16)
        for m in range(micros):
            for c in range(toks // 2):
                at = (m * toks + 2 * c) * tk
                vt = vbuf[kslot, at:at + 2 * tk, :]
                n = m * toks + 2 * c
                w2 = jnp.concatenate([jnp.concatenate([ws[n], zero], axis=1), jnp.concatenate([zero, ws[n + 1]], axis=1)], axis=0)
                o2 = mm(w2, vt)
                for u in range(2):
                    o_ht[m, pl.ds(2 * c + u, heads, stride=toks), :] = o2[u * heads:(u + 1) * heads] + own_w[n + u] * vals[n + u]
        for m in range(micros):
            for b in range(qw // 128):
                pieces = []
                for p in range(128 // head):
                    base = head_row(b * (128 // head) + p)
                    pieces.append(o_ht[m, base:base + toks, :])
                o_s[m * toks:(m + 1) * toks, b * 128:(b + 1) * 128] = jnp.concatenate(pieces, axis=1).astype(BF16)

        attn_out(i)
        for cp in new_copies(i):
            cp.start()

    def attn_out(i):
        span = 512
        mslot = lax.rem(i, SLOTS)
        attn = o_s[...]
        for n in range(width // span):
            part = mm(attn, wo[:, n * span:(n + 1) * span])
            h_mid[mslot, :, n * span:(n + 1) * span] = (h_buf[i, :, n * span:(n + 1) * span].astype(F32) + part).astype(BF16)
        rows_buf[mslot, place(me), :, 0:width] = rms(h_mid[mslot].astype(F32), mg_ref[...].astype(F32))
        rows_buf[mslot, place(me), :, width:width + 128] = msk_ref[i]

    def send_rows(i):
        for way in (1, 3, 2, 4, 0):
            ag_copy(i, way).start()

    def relay(i):
        for way in (1, 2):
            ag_copy(i, 2 * way - 1).wait_recv()
            relay_copy(i, way).start()

    def relay_near(i):
        for way in (1, 2):
            ag_copy(i, 2 * way).wait_recv()
            fw_copy(i, way - 1).start()

    def relay_far(i):
        for way in (1, 2):
            relay_copy(i, way).wait_recv()
        fw_copy(i, 2).start()

    def experts_up_first(j):
        slot = lax.rem(j, SLOTS)
        ag_copy(j, 0).wait_recv()
        for way in range(3):
            fw_copy(j, way).wait_recv()

        @pl.when(j == 0)
        def _():
            for e in range(local_e):
                for cp in ecopies(e):
                    cp.wait()

        total = ep_size * rows
        xs = rows_buf[slot, :, :, 0:width].reshape(total, width)
        experts = wr_ref.shape[0]
        logits = lax.dot_general(xs, wr_ref[...], (((1,), (1,)), ((), ())), preferred_element_type=F32)
        chosen = rows_buf[slot, :, :, width:width + 128].reshape(total, 128)[:, :experts].astype(F32) > 0.5
        logits = jnp.where(chosen, logits, -jnp.inf)
        numer = jnp.exp(logits - jnp.max(logits, axis=-1, keepdims=True))
        gates = numer / jnp.sum(numer, axis=-1, keepdims=True)
        lane = lax.broadcasted_iota(jnp.int32, (total, experts), 1)
        for e in range(local_e):
            col = jnp.sum(jnp.where(lane == me * local_e + e, gates, 0.0), axis=-1, keepdims=True)
            col_s[e] = jnp.broadcast_to(col, (total, 128))

        experts_up(j, range(UP_FIRST))

    def experts_up(j, group):
        slot = lax.rem(j, SLOTS)
        ff = wg.shape[2]
        xs = rows_buf[slot, :, :, 0:width].reshape(ep_size * rows, width)
        for e in group:
            for n in range(ff // 256):
                gate_h = mm(xs, wg[e, :, n * 256:(n + 1) * 256])
                up_h = mm(xs, wu[e, :, n * 256:(n + 1) * 256])
                act_s[e, :, n * 256:(n + 1) * 256] = (jax.nn.silu(gate_h) * up_h).astype(BF16)

    def pair_sum(j, p):
        half = lax.rem(j, 2)

        def both(dx, lo, hi):
            x = lax.rem(chip + dx, chips)
            return acc[p, core, :, x, lo:hi, :] + pair_buf[half, p, :, x, lo:hi, :]

        pair_copy(j, p).wait()
        c_send[half, 0, p, 0] = both(2, 0, mid)
        c_send[half, 0, p, 1] = both(2, mid, rows)
        for way in range(2):
            c_copy(j, p, 0, way).start()
        c_send[half, 1, p, 0] = both(1, mid, rows)
        c_send[half, 1, p, 1] = both(3, 0, mid)
        for way in range(2):
            c_copy(j, p, 1, way).start()
        c_send[half, 2, p, 0] = both(1, 0, mid)
        c_send[half, 2, p, 1] = both(3, mid, rows)
        c_own[half, p] = both(0, 0, rows)

    def sent_rows(j):
        for way in range(5):
            ag_copy(j, way).wait_send()
        for way in range(3):
            fw_copy(j, way).wait_send()
        for way in (1, 2):
            relay_copy(j, way).wait_send()

    def experts_down(j, p):
        for c in range(per):
            at = (p * per + c) * CHUNK
            for e in range(local_e):
                part = mm(act_s[e], wd[e, :, at:at + CHUNK])
                col = jnp.concatenate([col_s[e]] * (CHUNK // 128), axis=1)
                term = (col * part).astype(BF16).astype(F32).reshape(2, chips, rows, CHUNK)
                for k in range(2):
                    acc[p, k, c] = term[k] if e == 0 else acc[p, k, c] + term[k]
        pair_copy(j, p).start()

    def pass_on(j, p):
        half = lax.rem(j, 2)
        slot = lax.rem(j, SLOTS)
        for way in range(2):
            c_copy(j, p, 0, way).wait_recv()
            c_send[half, 2, p, way] = c_send[half, 2, p, way] + c_recv[slot, 0, p, way]
            c_copy(j, p, 2, way).start()

    def finish(j):
        slot = lax.rem(j, SLOTS)
        half = lax.rem(j, 2)
        for p in range(PARTS):
            for way in range(2):
                c_copy(j, p, 0, way).wait_send()
                c_copy(j, p, 1, way).wait()
                c_copy(j, p, 2, way).wait()
        parts = []
        for p in range(PARTS):
            for c in range(per):
                upper = c_recv[slot, 2, p, 0, c] + c_recv[slot, 1, p, 1, c]
                lower = c_recv[slot, 1, p, 0, c] + c_recv[slot, 2, p, 1, c]
                total = c_own[half, p, c] + jnp.concatenate([upper, lower], axis=0)
                at = (p * per + c) * CHUNK
                parts.append((h_mid[slot, :, at:at + CHUNK].astype(F32) + total.astype(BF16).astype(F32)).astype(BF16))
        hid = jnp.concatenate(parts, axis=1)

        @pl.when(stage < last)
        def _():
            h_out[j] = hid
            h_copy(j).start()

        @pl.when(stage == last)
        def _():
            h_out[j] = rms(hid.astype(F32), fg_ref[...].astype(F32).reshape(1, width))
            for d in sorted(range(1, pp_size), key=lambda d: -min(d, pp_size - d)):
                f_copy(j, d).start()
            f_local(j).start()

    def head_sum(j):
        pair_sum(j, 0)

    def tail_sum(j):
        pair_sum(j, 1)

    def head_on(j):
        pass_on(j, 0)

    def tail_on(j):
        pass_on(j, 1)

    def up_first(j):
        experts_up_first(j)

    def up_rest(j):
        experts_up(j, range(UP_FIRST, local_e))

    def down_head(j):
        sent_rows(j)
        experts_down(j, 0)

    def down_tail(j):
        experts_down(j, 1)

    order = (
        (attn_proj, 0),
        (relay_far, 1),
        (tail_sum, 2),
        (attn_core, 0),
        (send_rows, 0),
        (head_on, 2),
        (up_first, 1),
        (tail_on, 2),
        (up_rest, 1),
        (relay, 0),
        (down_head, 1),
        (relay_near, 0),
        (finish, 2),
        (down_tail, 1),
        (head_sum, 1),
    )

    def step(i, carry):
        for phase, lag in order:
            @pl.when((i >= lag) & (i < steps + lag))
            def _(phase=phase, lag=lag):
                phase(i - lag)

        return carry

    lax.fori_loop(0, steps + max(lag for _, lag in order), step, 0)

    for i in range(max(steps - 2, 0), steps):
        for cp in new_copies(i):
            cp.wait()

    def drain(j, carry):
        @pl.when(stage < last)
        def _():
            h_copy(j).wait_send()
            f_copy(j, 1).wait_recv()

        @pl.when(stage == last)
        def _():
            for d in range(1, pp_size):
                f_copy(j, d).wait_send()
            f_local(j).wait()

        return carry

    lax.fori_loop(0, steps, drain, 0)


def copy_kernel(count, *refs):
    src, dst, buf, in_sem, out_sem = refs[:count], refs[count:2 * count], refs[2 * count:3 * count], refs[-2], refs[-1]
    ins = [pltpu.make_async_copy(src[n], buf[n], in_sem.at[n]) for n in range(count)]
    outs = [pltpu.make_async_copy(buf[n], dst[n], out_sem.at[n]) for n in range(count)]
    for cp in ins:
        cp.start()
    for n in range(count):
        ins[n].wait()
        outs[n].start()
    for cp in outs:
        cp.wait()


def solution(mesh):
    ep_size = mesh.shape["ep"]
    pp_size = mesh.shape["pp"]
    rows_spec = ("dp", "ep")
    three_dim = P("pp", None, None)
    two_dim = P("pp", None)
    expert_spec = P("pp", "ep", None, None)
    cache_spec = P("pp", None, rows_spec, None, None, None)
    new_spec = P("pp", None, rows_spec, None, None)
    in_specs = (P(None, rows_spec, None), P(None, rows_spec), cache_spec, cache_spec, P("pp", None, rows_spec, None), three_dim, three_dim, three_dim, three_dim, two_dim, two_dim, three_dim, expert_spec, expert_spec, expert_spec, P(None))
    out_specs = (P(None, rows_spec, None), new_spec, new_spec)

    def device_fn(hidden_in, seq_pos, k_cache, v_cache, expert_ids, w_query, w_key, w_value, w_out, attn_gain, mlp_gain, w_router, w_gate, w_up, w_down, final_gain):
        assert w_query.shape[0] == 1
        micro_count, toks, width = hidden_in.shape
        ctx, kv_heads, head = k_cache.shape[3:]
        heads = w_query.shape[2] // head
        local_e, ff = w_gate.shape[1], w_gate.shape[3]
        kvw, qw = kv_heads * head, heads * head
        steps = micro_count // GROUP
        rows = GROUP * toks
        chips = ep_size // 2
        half = head // 2
        inv_freq = np.float32(THETA) ** (-np.arange(half, dtype=np.float32) / np.float32(half))
        ang = (np.arange(ctx + 1, dtype=np.float32)[:, None] * inv_freq).astype(np.float32)
        cos, sin = np.cos(ang), np.sin(ang)
        reps = 128 // head
        table = jnp.asarray(np.stack([np.concatenate([cos, cos] * reps, axis=-1), np.concatenate([-sin, sin] * reps, axis=-1)], axis=1), F32)
        ids = expert_ids[0].reshape(steps, rows, -1)
        chosen = jnp.max((ids[..., :, None] == jnp.arange(128, dtype=jnp.int32)).astype(BF16), axis=-2)
        cache_rows = GROUP * toks * ctx * kv_heads
        hrows = toks * heads
        per = width // CHUNK // PARTS
        cfg = (steps, rows, width, ep_size, pp_size, heads, kv_heads, head, ctx, toks, local_e)
        vm = pl.BlockSpec(memory_space=pltpu.VMEM)
        hb = pl.BlockSpec(memory_space=pl.ANY)
        dma = pltpu.SemaphoreType.DMA
        call = pl.pallas_call(
            functools.partial(kernel, cfg),
            out_shape=(jax.ShapeDtypeStruct((steps, rows, width), BF16),
                       jax.ShapeDtypeStruct((steps, rows, kv_heads, head), BF16),
                       jax.ShapeDtypeStruct((steps, rows, kv_heads, head), BF16)),
            in_specs=[pl.BlockSpec(memory_space=pltpu.SMEM), hb, vm, vm, hb, hb] + [hb] * 7 + [vm] * 4,
            out_specs=(hb, hb, hb),
            scratch_shapes=[
                pltpu.VMEM((width, qw + 2 * kvw), BF16), pltpu.VMEM((qw, width), BF16),
                pltpu.VMEM((local_e, width, ff), BF16), pltpu.VMEM((local_e, width, ff), BF16), pltpu.VMEM((local_e, ff, width), BF16),
                pltpu.VMEM((steps, rows, width), BF16), pltpu.VMEM((steps, rows, width), BF16), pltpu.VMEM((SLOTS, rows, width), BF16),
                pltpu.VMEM((SLOTS, ep_size, rows, width + 128), BF16),
                pltpu.VMEM((PARTS, 2, per, chips, rows, CHUNK), F32), pltpu.VMEM((2, PARTS, per, chips, rows, CHUNK), F32),
                pltpu.VMEM((2, 3, PARTS, 2, per, rows // 2, CHUNK), F32), pltpu.VMEM((2, PARTS, per, rows, CHUNK), F32), pltpu.VMEM((SLOTS, 3, PARTS, 2, per, rows // 2, CHUNK), F32),
                pltpu.VMEM((2, cache_rows, head), BF16), pltpu.VMEM((2, cache_rows, head), BF16),
                pltpu.VMEM((2, 2, rows, kv_heads, head), BF16), pltpu.VMEM((2, rows, 128), F32), pltpu.VMEM((GROUP, hrows + 2 * kv_heads * toks, head), F32), pltpu.VMEM((GROUP, hrows, head), F32), pltpu.VMEM((rows, qw), BF16),
                pltpu.VMEM((local_e, ep_size * rows, ff), BF16), pltpu.VMEM((local_e, ep_size * rows, 128), F32),
                dma((4,)), dma((3, local_e)), dma(()), dma((2, 2)), dma((2, 2)),
                dma((SLOTS, 5)), dma((SLOTS, 5)), dma((SLOTS, 2)), dma((SLOTS, 2)), dma((SLOTS, 3)), dma((SLOTS, 3)), dma((PARTS,)), dma((2, PARTS)), dma((2, 3, PARTS, 2)), dma((SLOTS, 3, PARTS, 2)),
                dma((steps,)), dma((steps,)), dma((steps, pp_size - 1)), dma((steps,)), dma((steps,)),
            ],
            compiler_params=pltpu.CompilerParams(collective_id=0, has_side_effects=True, vmem_limit_bytes=66 * 1000 * 1000),
        )
        out, k_new, v_new = call(
            seq_pos.T, hidden_in.reshape(steps, rows, width), table, chosen,
            k_cache.reshape(steps, cache_rows, head), v_cache.reshape(steps, cache_rows, head),
            w_query[0], w_key[0], w_value[0], w_out[0], w_gate[0], w_up[0], w_down[0], w_router[0].T,
            attn_gain, mlp_gain, final_gain)
        results = (out, k_new, v_new)
        out, k_new, v_new = pl.pallas_call(
            functools.partial(copy_kernel, len(results)),
            out_shape=[jax.ShapeDtypeStruct(r.shape, r.dtype) for r in results],
            in_specs=[hb] * len(results), out_specs=[hb] * len(results),
            scratch_shapes=[pltpu.VMEM(r.shape, r.dtype) for r in results] + [dma((len(results),))] * 2,
        )(*results)
        new_shape = (1, micro_count, toks, kv_heads, head)
        return out.reshape(micro_count, toks, width), k_new.reshape(new_shape), v_new.reshape(new_shape)

    return jax.shard_map(device_fn, mesh=mesh, in_specs=in_specs, out_specs=out_specs, check_vma=False)
```
